128 devices in a mesh: order: 32 (over y, x, core), help: 4 (over z).
Axes of the slice: x: 4, y: 4, z: 4, core: 2. Of those that a mesh axis runs over, the one named last changes fastest.
Arguments:
- raw_feats: bfloat16 [128, 1024, 256], P(('order', 'help')), may hold values from -6 to 6
- serial: int32 [128, 1024], P(('order', 'help')), may hold values from 0 to 1023, each once within a row
- counts: int32 [128, 1], P(('order', 'help')), may hold values from 1 to 1024, as said below
- norm_gain: float32 [256], replicated, may hold values from 0.1 to 1.9
- w_qkv: bfloat16 [256, 768], replicated
- w_proj: bfloat16 [256, 256], replicated, may hold values from -0.375 to 0.375
- out_grad: bfloat16 [128, 1024, 256], P(('order', 'help')), may hold values from -6 to 6
- cluster: int32 [128, 1024], P(('order', 'help')), may hold values from 0 to 255, never falling along the last dimension, each value on 1 to 8 neighbouring positions
- joined: int32 [128], P(('order', 'help')), may hold values 0 or 1
Outputs:
- pooled: bfloat16 [128, 1024, 256], P(('order', 'help'))
- grad_feats: bfloat16 [128, 1024, 256], P(('order', 'help'))
- grad_qkv: float32 [256, 768], replicated
- grad_proj: float32 [256, 256], replicated
- grad_gain: float32 [256], replicated
The draws below stay inside these ranges and needn't reach their ends.
Inputs may be any that keep to these rules, and one draw needn't show every extreme that they name: `serial`: each row is an ordering of the stored indices 0 to 1023. `counts`: the live points of a patch are its first ones. `cluster`: within a row, numbers start at 0, never fall, rise by at most one, and each number covers 1 to 8 points.
All inputs are finite; a program needn't handle non-finite values. No bound on the sum of `joined` on one device may be relied on, other than what follows from the above.
Results may differ from the reference program's by a relative error of at most 0.013.
The reference program's roundings to bfloat16 on the way (of `gathered`, `hidden`, `packed`, `weights`, `attended`, `block_out`, `back_proj` and `grad_packed`) count: a program that leaves them out, or rounds other values in their place, can miss the bound.
Values may be sent and summed in bfloat16 or wider, within the bound.
A program may use at most 192 MiB of HBM per device.

```python
import math
from functools import partial
import jax
import jax.numpy as jnp
import numpy as np
from jax import lax

C = 256
H = 16
PATCH = 1024
PATCHES_DEV = 1
GROUP = 8
ROWS = 1024
SHARDS = 128
POINTS = 131072


def draw_counts(key, part):
    dense_key, size_key, pick_key = jax.random.split(key, 3)
    dense_flag = jax.random.randint(dense_key, (SHARDS, 1), 0, 4) == 0
    forced_one = jnp.arange(SHARDS)[:, None] == jax.random.randint(pick_key, (), 0, SHARDS)
    sparse_sizes = jax.random.randint(size_key, (SHARDS, PATCHES_DEV), 1, PATCH // 2 + 1)
    return jnp.where(dense_flag | forced_one, PATCH, sparse_sizes).astype(jnp.int32)


def draw_w_qkv(key, part):
    base_key = jax.random.fold_in(key, 0)
    base_draw = jax.random.normal(base_key, (C, 3 * C), jnp.float32)
    column = jnp.arange(3 * C)
    column_scale = jnp.where(column < 2 * C, 2.0, 1.0) * C ** (-0.5)
    return (base_draw * column_scale[None, :]).astype(jnp.bfloat16)


def set_ends(result, rng, least, high):
    place = [jax.random.randint(jax.random.fold_in(rng, axis), (), 0, length) for axis, length in enumerate(result.shape)]
    main_axis = result.shape.index(max(result.shape))
    next_to = place[:main_axis] + [(place[main_axis] + 1) % result.shape[main_axis]] + place[main_axis + 1:]
    return result.at[tuple(place)].set(least).at[tuple(next_to)].set(high)


def shard_levels(stream_key, dims, cuts, low, high):
    factor_of, own = 1.0, jax.random.fold_in(stream_key, 6)
    for axis_at, blocks in cuts:
        heights = jnp.exp(jax.random.uniform(jax.random.fold_in(own, axis_at), (blocks,), jnp.float32, low / len(cuts), high / len(cuts)))
        factor_of = factor_of * jnp.repeat(heights, dims[axis_at] // blocks).reshape([-1 if axis == axis_at else 1 for axis in range(len(dims))])
    return factor_of


def split_up(count, total, reach, lean):
    loads = [(1 << 20) // math.isqrt(standing ** lean) + 1 for standing in range(2, count + 1)]
    surplus, holding = total - reach - (count - 1), [1] * (count - 1)
    while surplus > 0:
        candidates = [i for i in range(count - 1) if holding[i] < reach]
        whole, budget = sum([loads[i] for i in candidates]), surplus
        for i in candidates:
            extra = min(reach - holding[i], max(1, budget * loads[i] // whole), surplus)
            holding[i] = holding[i] + extra
            surplus = surplus - extra
    return np.array([reach] + holding)


def uneven(rng, amount, total, bound, lean):
    if amount == 2:
        one = jax.random.randint(rng, (), max(1, total - bound), min(bound, total - 1) + 1)
        return jnp.stack([one, total - one])
    lengths = jnp.asarray(split_up(amount, total, bound, lean), jnp.int32)
    twos = (amount - 1) // 2
    source_of, taker = lengths[1:1 + 2 * twos:2], lengths[2:2 + 2 * twos:2]
    margin = jnp.minimum(source_of - 1, bound - taker)
    moved = jax.random.randint(jax.random.fold_in(rng, 1), (twos,), 0, 1 << 20) % (margin + 1)
    lengths = lengths.at[1:1 + 2 * twos:2].set(source_of - moved).at[2:2 + 2 * twos:2].set(taker + moved)
    return lengths[jax.random.permutation(jax.random.fold_in(rng, 2), amount)]


def normal_values(stream_key, shape, spread, limit, cuts=(), held_as=jnp.bfloat16):
    array = jax.random.normal(stream_key, shape, jnp.float32) * spread
    if len(cuts) > 0:
        array = shard_levels(stream_key, shape, cuts, -0.22, 0.18) * array
    return jnp.clip(array, min=-limit, max=limit).astype(held_as)


def setup_inputs(seed: int = 0) -> dict:
    key_of = jax.random.split(jax.random.key(seed), 10)
    raw_feats = normal_values(key_of[0], (SHARDS, ROWS, C), 1.0, 6.0, ((0, 128),))
    serial = jax.vmap(lambda own: jax.random.permutation(own, ROWS))(jax.random.split(key_of[1], SHARDS)).reshape((SHARDS, ROWS)).astype(jnp.int32)
    counts = draw_counts(jax.random.fold_in(key_of[9], 71), 0)
    norm_gain = jnp.clip(1.0 + 0.18 * jax.random.normal(key_of[3], (C,), jnp.float32), 0.1, 1.9)
    w_qkv = draw_w_qkv(jax.random.fold_in(key_of[9], 71), 0)
    w_proj = normal_values(key_of[5], (C, C), C ** -0.5, 0.375)
    out_grad = normal_values(key_of[6], (SHARDS, ROWS, C), 1.0, 6.0, ((0, 128),))
    cluster = jax.vmap(lambda own: jnp.searchsorted(jnp.cumsum(uneven(own, ROWS // 4, ROWS, GROUP, 0)), jnp.arange(ROWS), side="right"))(jax.random.split(key_of[7], SHARDS)).reshape((SHARDS, ROWS)).astype(jnp.int32)
    joined = set_ends((jax.random.randint(key_of[8], (SHARDS,), 0, 2) < 1).astype(jnp.int32), jax.random.fold_in(key_of[8], 1), 0, 1)
    return dict(raw_feats=raw_feats, serial=serial, counts=counts, norm_gain=norm_gain, w_qkv=w_qkv, w_proj=w_proj, out_grad=out_grad, cluster=cluster, joined=joined)


EPS = 1e-05
NEG = -1e+30

def head_block(queries, key_rows, value_rows, alive_mask):
    score_scale = queries.shape[-1] ** (-0.5)
    scores = jnp.einsum('qhd,khd->hqk', queries, key_rows, preferred_element_type=jnp.float32) * score_scale
    scores = jnp.where(alive_mask[None, None, :], scores, NEG)
    row_peak = lax.optimization_barrier(jnp.max(scores, axis=-1, keepdims=True))
    exp_terms = jnp.exp(scores - row_peak)
    weights = (exp_terms / lax.optimization_barrier(jnp.sum(exp_terms, axis=-1, keepdims=True))).astype(jnp.bfloat16)
    mixed_out = jnp.einsum('hqk,khd->qhd', weights, value_rows, preferred_element_type=jnp.float32)
    return jnp.where(alive_mask[:, None, None], mixed_out, 0.0).astype(jnp.bfloat16)

def attend_patch(qkv_in, count_in, head_size):
    checked_block = jax.checkpoint(head_block)
    row_total = qkv_in.shape[0]
    chan_width = qkv_in.shape[2]
    heads_here = chan_width // head_size
    group_heads = min(4, heads_here)
    alive_mask = jnp.arange(row_total, dtype=jnp.int32) < count_in
    blocks = qkv_in.reshape(row_total, 3, heads_here // group_heads, group_heads, head_size).transpose(2, 0, 1, 3, 4)

    def one_block(head_group):
        return checked_block(head_group[:, 0], head_group[:, 1], head_group[:, 2], alive_mask)
    mixed_out = lax.map(one_block, blocks)
    return mixed_out.transpose(1, 0, 2, 3).reshape(row_total, chan_width)

def attend_all(qkv_in, patch_counts, head_size):

    def per_patch(operands):
        return attend_patch(operands[0], operands[1], head_size)
    return lax.map(per_patch, (qkv_in, patch_counts))

def layer_stats(rows_in):
    values = rows_in.astype(jnp.float32)
    centred = values - lax.optimization_barrier(jnp.mean(values, axis=-1, keepdims=True))
    inv_std = lax.rsqrt(lax.optimization_barrier(jnp.mean(centred * centred, axis=-1, keepdims=True)) + EPS)
    return (centred * inv_std, inv_std)

def norm_backward(grad_norm, normed, inv_std):
    mean_grad = lax.optimization_barrier(jnp.mean(grad_norm, axis=-1, keepdims=True))
    mean_cross = lax.optimization_barrier(jnp.mean(grad_norm * normed, axis=-1, keepdims=True))
    return inv_std * (grad_norm - mean_grad - normed * mean_cross)

def reference(raw_feats, serial, counts, norm_gain, w_qkv, w_proj, out_grad, cluster, joined):
    chan_width = raw_feats.shape[-1]
    head_size = chan_width // H
    gathered = jnp.take_along_axis(raw_feats, serial[:, :, None], axis=1).reshape(POINTS, chan_width)
    normed, inv_std = layer_stats(gathered)
    hidden = (normed * norm_gain).astype(jnp.bfloat16)
    packed = jnp.dot(hidden, w_qkv, preferred_element_type=jnp.float32).astype(jnp.bfloat16)
    packed = packed.reshape(POINTS // PATCH, PATCH, 3, chan_width)
    grad_out = out_grad.reshape(POINTS, chan_width)
    back_proj = jnp.einsum('nd,cd->nc', grad_out, w_proj, preferred_element_type=jnp.float32).astype(jnp.bfloat16)
    attend_fixed = partial(attend_all, patch_counts=counts.reshape(-1), head_size=head_size)
    own_out, pullback = jax.vjp(attend_fixed, packed)
    grad_packed = pullback(back_proj.reshape(POINTS // PATCH, PATCH, chan_width))[0]
    attended = own_out.reshape(POINTS, chan_width)
    block_out = (gathered.astype(jnp.float32) + jnp.dot(attended, w_proj, preferred_element_type=jnp.float32)).astype(jnp.bfloat16)
    seg_total = (cluster[:, -1] + 1).astype(jnp.int32)
    link_flags = joined.at[0].set(0).astype(jnp.int32)
    seg_start = (jnp.cumsum(seg_total) - seg_total - jnp.cumsum(link_flags)).astype(jnp.int32)
    global_ids = (cluster + seg_start[:, None]).astype(jnp.int32).reshape(-1)
    group_max = jax.ops.segment_max(block_out, global_ids, num_segments=POINTS)
    pooled = jnp.take(group_max, global_ids, axis=0).reshape(SHARDS, ROWS, chan_width)
    grad_flat = grad_packed.reshape(POINTS, 3 * chan_width)
    grad_hidden = jnp.einsum('nk,ck->nc', grad_flat, w_qkv, preferred_element_type=jnp.float32)
    point_scale = 2.0 * ROWS ** (-0.5)
    grad_qkv = jnp.einsum('nc,nk->ck', hidden, grad_flat, preferred_element_type=jnp.float32) * point_scale
    grad_proj = jnp.einsum('nc,nd->cd', attended, grad_out, preferred_element_type=jnp.float32) * point_scale
    grad_gain = lax.optimization_barrier(jnp.sum(grad_hidden * normed, axis=0)) * point_scale
    grad_input = (grad_out.astype(jnp.float32) + norm_backward(grad_hidden * norm_gain, normed, inv_std)).astype(jnp.bfloat16)
    shard_index = jnp.arange(SHARDS, dtype=jnp.int32)[:, None]
    inverse = jnp.zeros((SHARDS, ROWS), jnp.int32).at[shard_index, serial].set(jnp.arange(ROWS, dtype=jnp.int32)[None, :])
    grad_feats = jnp.take_along_axis(grad_input.reshape(SHARDS, ROWS, chan_width), inverse[:, :, None], axis=1)
    return (pooled, grad_feats, grad_qkv, grad_proj, grad_gain)
```

```python
import math

import jax
import jax.numpy as jnp
from jax import lax
from jax.experimental import pallas as pl
from jax.experimental.pallas import tpu as pltpu
from jax.sharding import Mesh
from jax.sharding import PartitionSpec as P

H = 16
C = 256
N = 1024
HD = 16
QB = 256
NQ = N // QB
GROUP = 8
ORDER_HELP = ("order_0", "order_1", "order_2", "help")
EPS = 1e-05
NEG = -1e30
SCALE = HD**-0.5
QSCALE = SCALE * math.log2(math.e)
POINT_SCALE = 2.0 * N**-0.5
F32 = jnp.float32
BF16 = jnp.bfloat16
MESH = pl.DeviceIdType.MESH
VMEM = pltpu.VMEM


def iota(shape, dim):
    return lax.broadcasted_iota(jnp.int32, shape, dim)


def mm(a, b):
    return jnp.dot(a, b, preferred_element_type=F32)


def mm_nt(a, b):
    return lax.dot_general(a, b, (((1,), (1,)), ((), ())), preferred_element_type=F32)


def split3(x):
    hi = x.astype(BF16)
    rest = x - hi.astype(F32)
    mid = rest.astype(BF16)
    lo = (rest - mid.astype(F32)).astype(BF16)
    return hi, mid, lo


def local_kernel(
    raw_ref,
    serial_ref,
    counts_ref,
    gain_ref,
    wqkv_ref,
    wproj_ref,
    og_ref,
    cluster_ref,
    pooled_ref,
    gfeats_ref,
    send_ref,
    gsum_ref,
    edge_ref,
    gath_ref,
    hid_ref,
    normed_ref,
    inv_ref,
    pT_ref,
    doT_ref,
    ka_ref,
    va_ref,
    qa_ref,
    vt_ref,
    e_ref,
    ds_ref,
    attT_ref,
    gpT_ref,
    dk_ref,
    dv_ref,
    grad_ref,
    dx_ref,
    bo_ref,
):
    n_live = counts_ref[0, 0]
    gain = gain_ref[...]
    serial_row = serial_ref[...]
    serial_cols = jnp.transpose(jnp.broadcast_to(serial_row.astype(F32), (128, N)))
    lane128 = iota((QB, 128), 1).astype(F32)

    for t in range(4):
        rows = pl.ds(t * QB, QB)
        sc = serial_cols[t * QB : (t + 1) * QB]
        onehot = jnp.concatenate(
            [jnp.where(sc == lane128 + float(128 * b), 1.0, 0.0).astype(BF16) for b in range(8)],
            axis=1,
        )
        x = mm(onehot, raw_ref[...])
        gath_ref[rows, :] = x.astype(BF16)
        centred = x - jnp.mean(x, axis=1, keepdims=True)
        inv = lax.rsqrt(jnp.mean(centred * centred, axis=1, keepdims=True) + EPS)
        normed = centred * inv
        normed_ref[rows, :] = normed
        inv_ref[rows, :] = inv
        hid = (normed * gain).astype(BF16)
        hid_ref[rows, :] = hid
        packed = mm(hid, wqkv_ref[...]).astype(BF16)
        pT_ref[:, rows] = jnp.transpose(packed)
        bp = mm_nt(og_ref[rows, :], wproj_ref[...]).astype(BF16)
        bpT = jnp.transpose(bp)
        lane = iota((C, QB), 1) + t * QB
        doT_ref[:, rows] = jnp.where(lane < n_live, bpT.astype(F32), 0.0).astype(BF16)
        key_live = (iota((QB, C), 0) + t * QB) < n_live
        kcols = packed[:, C : 2 * C]
        vcols = packed[:, 2 * C :]
        for b in range(4):
            cols = pl.ds(b * C, C)
            chan = iota((C, C), 0)
            place = iota((C, C), 1)
            spot = place % 64
            same = ((place // 64 + 4 * b) == chan // HD) & (spot % HD == chan % HD)
            rep_k = jnp.where(same & (spot < 3 * HD), 1.0, 0.0).astype(BF16)
            rep_v = jnp.where(same & (spot < 2 * HD), 1.0, 0.0).astype(BF16)
            spot_r = iota((QB, C), 1) % 64
            ka = mm(kcols, rep_k)
            ka = jnp.where((spot_r >= 48) & (spot_r < 51), 1.0, ka)
            ka = jnp.where((spot_r == 51) & jnp.logical_not(key_live), NEG, ka)
            ka_ref[rows, cols] = ka.astype(BF16)
            va = mm(vcols, rep_v)
            va = jnp.where((spot_r >= 32) & (spot_r < 35), 1.0, va)
            va_ref[rows, cols] = va.astype(BF16)

    def prep(h, carry):
        q = pT_ref[pl.ds(h * HD, HD), :].astype(F32)
        k = pT_ref[pl.ds(C + h * HD, HD), :].astype(F32)
        v = pT_ref[pl.ds(2 * C + h * HD, HD), :]
        do = doT_ref[pl.ds(h * HD, HD), :]
        q = q * QSCALE
        hi, mid, lo = split3(q)
        row = iota((HD, N), 0)
        tail = jnp.where(row == 3, 1.0, 0.0).astype(BF16)
        zeros = jnp.zeros((64, N), BF16)
        base = pl.multiple_of(h * 128, 128)
        half = pl.multiple_of((h % 2) * 64, 64)
        qa_ref[pl.ds(pl.multiple_of(base + half, 64), 64), :] = jnp.concatenate(
            [hi, mid, lo, tail], axis=0
        )
        qa_ref[pl.ds(pl.multiple_of(base + 64 - half, 64), 64), :] = zeros
        ones = jnp.where(row == 0, 1.0, 0.0).astype(BF16)
        vt_ref[pl.ds(h * 32, 32), :] = jnp.concatenate([v, ones], axis=0)
        q2 = jnp.max(jnp.sum(q * q, axis=0, keepdims=True))
        k2 = jnp.max(jnp.sum(k * k, axis=0, keepdims=True))
        vmax = jnp.max(jnp.abs(v.astype(F32)))
        dmax = jnp.max(jnp.abs(do.astype(F32)))
        tame = (q2 * k2 <= 8100.0) & (vmax <= 4096.0) & (dmax <= 4096.0)

        @pl.when(jnp.logical_not(tame))
        def _():
            lanes = pl.ds(pl.multiple_of((h // 2) * 128, 128), 128)
            for t in range(NQ):
                cols = pl.ds(t * QB, QB)
                peak = jnp.full((1, QB), -jnp.inf, F32)
                for r in range(4):
                    s = mm(ka_ref[pl.ds(r * QB, QB), lanes], qa_ref[pl.ds(base, 128), cols])
                    peak = jnp.maximum(peak, jnp.max(s, axis=0, keepdims=True))
                p_hi, p_mid, p_lo = split3(-peak)
                rowq = iota((HD, QB), 0)
                shift = jnp.where(rowq == 0, p_hi.astype(F32), 0.0)
                shift = jnp.where(rowq == 1, p_mid.astype(F32), shift)
                shift = jnp.where(rowq == 2, p_lo.astype(F32), shift)
                shift = jnp.where(rowq == 3, 1.0, shift)
                at = pl.multiple_of(base + half + 48, 16)
                qa_ref[pl.ds(at, HD), cols] = shift.astype(BF16)

        return carry

    lax.fori_loop(0, H, prep, 0)

    def first_stage(p, j):
        side, t, slot = j // NQ, j % NQ, j % 2
        h = 2 * p + side
        lanes = pl.ds(pl.multiple_of(p * 128, 128), 128)
        rhs = qa_ref[pl.ds(pl.multiple_of(h * 128, 128), 128), t * QB : (t + 1) * QB]
        s = mm(ka_ref[:, lanes], rhs)
        e_ref[slot] = jnp.exp2(s).astype(BF16)

    def second_stage(p, j):
        side, t, slot = j // NQ, j % NQ, j % 2
        h = 2 * p + side
        cols = slice(t * QB, (t + 1) * QB)
        lanes = pl.ds(pl.multiple_of(p * 128, 128), 128)
        hrows = pl.ds(pl.multiple_of(h * HD, HD), HD)
        krows = pl.ds(pl.multiple_of(C + h * HD, HD), HD)
        vrows = pl.ds(pl.multiple_of(2 * C + h * HD, HD), HD)
        o_un = mm(vt_ref[pl.ds(pl.multiple_of(h * 32, 32), 32), :], e_ref[slot])
        l_inv = 1.0 / o_un[HD : HD + 1, :]
        o = o_un[:HD, :] * l_inv
        live = (iota((HD, QB), 1) + t * QB) < n_live
        attT_ref[hrows, cols] = jnp.where(live, o, 0.0).astype(BF16)
        do = doT_ref[hrows, cols].astype(F32)
        dl = do * l_inv
        d_hi = dl.astype(BF16)
        d_lo = (dl - d_hi.astype(F32)).astype(BF16)
        cross = -jnp.sum(dl * o, axis=0, keepdims=True)
        c_hi, c_mid, c_lo = split3(cross)
        row = iota((32, QB), 0)
        tail = jnp.where(row == 0, c_hi.astype(F32), 0.0)
        tail = jnp.where(row == 1, c_mid.astype(F32), tail)
        tail = jnp.where(row == 2, c_lo.astype(F32), tail)
        both = jnp.concatenate([d_hi, d_lo], axis=0)
        zeros = jnp.zeros((64, QB), BF16)
        parts = [both, tail.astype(BF16)]
        parts = parts + [zeros] if side == 0 else [zeros] + parts
        dp = mm(va_ref[:, lanes], jnp.concatenate(parts, axis=0))
        ds_ref[...] = (e_ref[slot].astype(F32) * dp).astype(BF16)
        dv = mm_nt(both, e_ref[slot])
        dv = dv[:HD] + dv[HD:]
        dq = mm(pT_ref[krows, :], ds_ref[...])
        gpT_ref[hrows, cols] = (dq * SCALE).astype(BF16)
        dk = mm_nt(pT_ref[hrows, cols], ds_ref[...])
        if t == 0:
            dk_ref[...] = dk
            dv_ref[...] = dv
        elif t < NQ - 1:
            dk_ref[...] += dk
            dv_ref[...] += dv
        else:
            gpT_ref[krows, :] = ((dk_ref[...] + dk) * SCALE).astype(BF16)
            gpT_ref[vrows, :] = (dv_ref[...] + dv).astype(BF16)

    first_stage(0, 0)

    def pair(p, carry):
        for j in range(2 * NQ):
            if j < 2 * NQ - 1:
                first_stage(p, j + 1)
            else:
                first_stage(jnp.minimum(p + 1, H // 2 - 1), 0)
            second_stage(p, j)
        return carry

    lax.fori_loop(0, H // 2, pair, 0)

    grad_ref[: 3 * C, :] = mm(gpT_ref[...], hid_ref[...]) * POINT_SCALE
    grad_ref[3 * C :, :] = mm(attT_ref[...], og_ref[...]) * POINT_SCALE
    for half in range(2):
        part = grad_ref[:, half * 128 : (half + 1) * 128].reshape(128, 8, 128)
        send_ref[:, half * 8 : (half + 1) * 8, :] = part.astype(BF16)

    gain_sum = jnp.zeros((1, C), F32)
    for t in range(4):
        rows = pl.ds(t * QB, QB)
        att = jnp.transpose(attT_ref[:, rows])
        bo = gath_ref[rows, :].astype(F32) + mm(att, wproj_ref[...])
        bo_ref[rows, :] = bo.astype(BF16).astype(F32)
        gp = jnp.transpose(gpT_ref[:, rows])
        gh = mm_nt(gp, wqkv_ref[...])
        normed = normed_ref[rows, :]
        gain_sum = gain_sum + jnp.sum(gh * normed, axis=0, keepdims=True)
        g = gh * gain
        mean_g = jnp.mean(g, axis=1, keepdims=True)
        mean_c = jnp.mean(g * normed, axis=1, keepdims=True)
        dx = og_ref[rows, :].astype(F32) + inv_ref[rows, :] * (g - mean_g - normed * mean_c)
        dx_ref[rows, :] = dx.astype(BF16)
    gain_sum = gain_sum * POINT_SCALE
    gsum_ref[0] = gain_sum[:, :128]
    gsum_ref[1] = gain_sum[:, 128:]
    for t in range(4):
        spot = iota((QB, N), 0) + t * QB
        onehot = jnp.where(spot == serial_row, 1.0, 0.0).astype(BF16)
        gfeats_ref[pl.ds(t * QB, QB), :] = mm(onehot, dx_ref[...]).astype(BF16)

    ids = jnp.transpose(jnp.broadcast_to(cluster_ref[...].astype(F32), (128, N)))
    row = iota((N, 128), 0)
    down_ok, up_ok = [], []
    for step in (1, 2, 4):
        down_ok.append((pltpu.roll(ids, step, 0) == ids) & (row >= step))
        up_ok.append((pltpu.roll(ids, N - step, 0) == ids) & (row < N - step))
    for half in range(2):
        cols = slice(half * 128, (half + 1) * 128)
        m = bo_ref[:, cols]
        for i, step in enumerate((1, 2, 4)):
            m = jnp.maximum(m, jnp.where(down_ok[i], pltpu.roll(m, step, 0), -jnp.inf))
        for i, step in enumerate((1, 2, 4)):
            m = jnp.maximum(m, jnp.where(up_ok[i], pltpu.roll(m, N - step, 0), -jnp.inf))
        pooled_ref[:, cols] = m.astype(BF16)
        edge_ref[0, :, cols] = m[:8]
        edge_ref[1, :, cols] = m[N - 8 :]


def local_part(raw, serial, counts, gain, w_qkv, w_proj, out_grad, cluster):
    shapes = (
        jax.ShapeDtypeStruct((N, C), BF16),
        jax.ShapeDtypeStruct((N, C), BF16),
        jax.ShapeDtypeStruct((128, 16, 128), BF16),
        jax.ShapeDtypeStruct((2, 1, 128), F32),
        jax.ShapeDtypeStruct((2, 8, C), F32),
    )
    vm = pl.BlockSpec(memory_space=VMEM)
    sm = pl.BlockSpec(memory_space=pltpu.SMEM)
    return pl.pallas_call(
        local_kernel,
        out_shape=shapes,
        in_specs=[vm, vm, sm, vm, vm, vm, vm, vm],
        out_specs=[vm] * 5,
        scratch_shapes=[
            VMEM((N, C), BF16),
            VMEM((N, C), BF16),
            VMEM((N, C), F32),
            VMEM((N, 1), F32),
            VMEM((3 * C, N), BF16),
            VMEM((C, N), BF16),
            VMEM((N, 4 * C), BF16),
            VMEM((N, 4 * C), BF16),
            VMEM((H * 128, N), BF16),
            VMEM((H * 32, N), BF16),
            VMEM((2, N, QB), BF16),
            VMEM((N, QB), BF16),
            VMEM((C, N), BF16),
            VMEM((3 * C, N), BF16),
            VMEM((HD, N), F32),
            VMEM((HD, N), F32),
            VMEM((N, C), F32),
            VMEM((N, C), BF16),
            VMEM((N, C), F32),
        ],
        compiler_params=pltpu.CompilerParams(vmem_limit_bytes=56 * 1024 * 1024),
        name="local_part",
    )(raw, serial, counts, gain, w_qkv, w_proj, out_grad, cluster)


def comm_kernel(
    send_ref,
    gsum_ref,
    edge_ref,
    pooled_in_ref,
    cluster_ref,
    joined_ref,
    pooled_ref,
    gqkv_ref,
    gproj_ref,
    ggain_ref,
    pair_buf,
    pair_gain,
    edge_buf,
    chip_buf,
    chip_gain,
    rs_buf,
    gain_buf,
    ag_buf,
    out_buf,
    gain_out,
    grad_buf,
    sems,
):
    y = lax.axis_index("order_0")
    x = lax.axis_index("order_1")
    core = lax.axis_index("order_2")
    z = lax.axis_index("help")
    chip = (y * 4 + x) * 4 + z
    shard = ((y * 4 + x) * 2 + core) * 4 + z

    def of_shard(s):
        return (s // 32, (s // 8) % 4, (s // 4) % 2, s % 4)

    def of_chip(r):
        return ((y + r // 16) % 4, (x + (r // 4) % 4) % 4, core, (z + r % 4) % 4)

    partner = (y, x, 1 - core, z)
    following = of_shard((shard + 1) % 128)
    previous = of_shard((shard + 127) % 128)

    barrier = pltpu.get_barrier_semaphore()

    def greet(r, carry):
        pl.semaphore_signal(barrier, inc=1, device_id=of_chip(r), device_id_type=MESH)
        return carry

    lax.fori_loop(1, 64, greet, 0)
    for other in (partner, following, previous):
        pl.semaphore_signal(barrier, inc=1, device_id=other, device_id_type=MESH)
    pl.semaphore_wait(barrier, 66)

    def remote(src, dst, i, device):
        return pltpu.make_async_remote_copy(
            src_ref=src,
            dst_ref=dst,
            send_sem=sems.at[2 * i],
            recv_sem=sems.at[2 * i + 1],
            device_id=device,
            device_id_type=MESH,
        )

    far = 64 * (1 - core)
    pair_copy = remote(send_ref.at[pl.ds(far, 64)], pair_buf, 0, partner)
    pair_copy.start()
    pair_gain_copy = remote(gsum_ref.at[1 - core], pair_gain, 1, partner)
    pair_gain_copy.start()
    ahead = remote(edge_ref.at[1], edge_buf.at[0], 2, following)
    ahead.start()
    back = remote(edge_ref.at[0], edge_buf.at[1], 3, previous)
    back.start()

    pair_copy.wait()
    mine = send_ref[pl.ds(64 * core, 64)].astype(F32) + pair_buf[...].astype(F32)
    chip_buf[...] = mine.astype(BF16)
    pair_gain_copy.wait()
    chip_gain[...] = gsum_ref[core] + pair_gain[...]

    def scatter(r, carry):
        to = of_chip(r)
        other = (to[0] * 4 + to[1]) * 4 + to[3]
        remote(chip_buf.at[other], rs_buf.at[chip], 4, to).start()
        remote(chip_gain, gain_buf.at[chip], 5, to).start()
        return carry

    lax.fori_loop(1, 64, scatter, 0)
    rs_buf[pl.ds(chip, 1)] = chip_buf[pl.ds(chip, 1)]
    gain_buf[pl.ds(chip, 1)] = chip_gain[...][None]

    ahead.wait()
    back.wait()
    ids = jnp.transpose(jnp.broadcast_to(cluster_ref[...].astype(F32), (128, N)))
    first = ids[:8]
    last = ids[N - 8 :]
    pooled_ref[...] = pooled_in_ref[...]
    row = iota((8, 128), 0)
    linked = (joined_ref[...] > 0) & (shard > 0)
    head_ok = (first == first[:1]) & linked
    next_joined = edge_buf[1, 8:9, :128] > 0.0
    tail_ok = (last == last[7:8]) & next_joined & (shard < 127)
    for half in range(2):
        cols = slice(half * 128, (half + 1) * 128)
        from_prev = edge_buf[0, 7:8, cols]
        from_next = edge_buf[1, 0:1, cols]
        top = edge_ref[0, 0:8, cols]
        top = jnp.where(head_ok, jnp.maximum(top, from_prev), top)
        low = edge_ref[1, 0:8, cols]
        low = jnp.where(tail_ok, jnp.maximum(low, from_next), low)
        pooled_ref[0:16, cols] = jnp.concatenate(
            [top, pooled_in_ref[8:16, cols].astype(F32)], axis=0
        ).astype(BF16)
        pooled_ref[N - 16 : N, cols] = jnp.concatenate(
            [pooled_in_ref[N - 16 : N - 8, cols].astype(F32), low], axis=0
        ).astype(BF16)

    everything = pl.ds(0, 63)
    for i, (src, dst) in ((4, (ag_buf, rs_buf)), (5, (gain_out, gain_buf))):
        whole = remote(dst.at[everything], dst.at[everything], i, partner)
        whole.wait_recv()
        whole.wait_send()
    total = jnp.sum(rs_buf[...].astype(F32), axis=0)
    ag_buf[pl.ds(chip, 1)] = total.astype(BF16)[None]

    def gather(r, carry):
        remote(ag_buf.at[chip], ag_buf.at[chip], 6, of_chip(r)).start()
        return carry

    lax.fori_loop(1, 64, gather, 0)
    gain_out[pl.ds(core, 1)] = jnp.sum(gain_buf[...], axis=0)[None]
    last_gain = remote(gain_out.at[core], gain_out.at[core], 7, partner)
    last_gain.start()
    whole = remote(ag_buf.at[everything], ag_buf.at[everything], 6, partner)
    whole.wait_recv()
    whole.wait_send()
    last_copy = remote(ag_buf, out_buf.at[core], 8, partner)
    last_copy.start()
    out_buf[pl.ds(core, 1)] = ag_buf[...][None]
    last_gain.wait()
    ggain_ref[:, :128] = gain_out[0]
    ggain_ref[:, 128:] = gain_out[1]
    last_copy.wait()
    for c in range(2):
        for half in range(2):
            part = out_buf[c, :, half * 8 : (half + 1) * 8, :].astype(F32).reshape(512, 128)
            grad_buf[c * 512 : (c + 1) * 512, half * 128 : (half + 1) * 128] = part
    gqkv_ref[...] = jnp.transpose(grad_buf[: 3 * C, :])
    gproj_ref[...] = grad_buf[3 * C :, :]


def comm_part(send, gsum, edge, pooled, cluster, joined):
    shapes = (
        jax.ShapeDtypeStruct((N, C), BF16),
        jax.ShapeDtypeStruct((C, 3 * C), F32),
        jax.ShapeDtypeStruct((C, C), F32),
        jax.ShapeDtypeStruct((1, C), F32),
    )
    vm = pl.BlockSpec(memory_space=VMEM)
    return pl.pallas_call(
        comm_kernel,
        out_shape=shapes,
        in_specs=[vm] * 6,
        out_specs=[vm] * 4,
        scratch_shapes=[
            VMEM((64, 16, 128), BF16),
            VMEM((1, 128), F32),
            VMEM((2, 16, C), F32),
            VMEM((64, 16, 128), BF16),
            VMEM((1, 128), F32),
            VMEM((64, 16, 128), BF16),
            VMEM((64, 1, 128), F32),
            VMEM((64, 16, 128), BF16),
            VMEM((2, 64, 16, 128), BF16),
            VMEM((2, 1, 128), F32),
            VMEM((N, C), F32),
            pltpu.SemaphoreType.DMA((18,)),
        ],
        compiler_params=pltpu.CompilerParams(
            collective_id=0, has_side_effects=True, vmem_limit_bytes=32 * 1024 * 1024
        ),
        name="comm_part",
    )(send, gsum, edge, pooled, cluster, joined)


def body(raw_feats, serial, counts, norm_gain, w_qkv, w_proj, out_grad, cluster, joined):
    pooled, grad_feats, send, gsum, edge = local_part(
        raw_feats[0], serial, counts, norm_gain[None], w_qkv, w_proj, out_grad[0], cluster
    )
    flag = jnp.broadcast_to(joined[:, None], (8, C)).astype(F32)
    edge = jnp.concatenate([edge, jnp.broadcast_to(flag, (2, 8, C))], axis=1)
    flags = jnp.broadcast_to(joined[:, None], (1, 128))
    pooled, grad_qkv, grad_proj, grad_gain = comm_part(send, gsum, edge, pooled, cluster, flags)
    return (pooled[None], grad_feats[None], grad_qkv, grad_proj, grad_gain[0])


def solution(mesh):
    torus = Mesh(
        mesh.devices.reshape(4, 4, 2, mesh.shape["help"]), ("order_0", "order_1", "order_2", "help")
    )
    placed = (
        P(ORDER_HELP, None, None),
        P(ORDER_HELP, None),
        P(ORDER_HELP, None),
        P(),
        P(),
        P(),
        P(ORDER_HELP, None, None),
        P(ORDER_HELP, None),
        P(ORDER_HELP),
    )
    return jax.shard_map(
        body,
        mesh=torus,
        in_specs=placed,
        out_specs=(P(ORDER_HELP, None, None), P(ORDER_HELP, None, None), P(), P(), P()),
        check_vma=False,
    )
```

```python
import math

import jax
import jax.numpy as jnp
from jax import lax
from jax.experimental import pallas as pl
from jax.experimental.pallas import tpu as pltpu
from jax.sharding import Mesh
from jax.sharding import PartitionSpec as P

H = 16
C = 256
N = 1024
HD = 16
QB = 256
NQ = N // QB
AQ = 512
NA = N // AQ
LAG = True
GROUP = 8
ORDER_HELP = ("order_0", "order_1", "order_2", "help")
EPS = 1e-05
NEG = -1e30
SCALE = HD**-0.5
QSCALE = SCALE * math.log2(math.e)
POINT_SCALE = 2.0 * N**-0.5
F32 = jnp.float32
BF16 = jnp.bfloat16
MESH = pl.DeviceIdType.MESH
VMEM = pltpu.VMEM


def iota(shape, dim):
    return lax.broadcasted_iota(jnp.int32, shape, dim)


def mm(a, b):
    return jnp.dot(a, b, preferred_element_type=F32)


def mm_nt(a, b):
    return lax.dot_general(a, b, (((1,), (1,)), ((), ())), preferred_element_type=F32)


def split3(x):
    hi = x.astype(BF16)
    rest = x - hi.astype(F32)
    mid = rest.astype(BF16)
    lo = (rest - mid.astype(F32)).astype(BF16)
    return hi, mid, lo


def local_kernel(
    raw_ref,
    serial_ref,
    counts_ref,
    gain_ref,
    wqkv_ref,
    wproj_ref,
    og_ref,
    cluster_ref,
    joined_ref,
    pooled_ref,
    gfeats_ref,
    send_ref,
    gsum_ref,
    edge_ref,
    gath_ref,
    hid_ref,
    normed_ref,
    inv_ref,
    pT_ref,
    doT_ref,
    ka_ref,
    va_ref,
    qa_ref,
    vt_ref,
    e_ref,
    ds_ref,
    attT_ref,
    gpT_ref,
    dk_ref,
    dv_ref,
    grad_ref,
    dx_ref,
    bo_ref,
    bo2_ref,
    ids_ref,
    cols_ref,
    kv_ref,
):
    n_live = counts_ref[0, 0]
    gain = gain_ref[...]
    serial_row = serial_ref[...]
    cols_ref[...] = jnp.transpose(jnp.broadcast_to(serial_row.astype(F32), (128, N)))
    lane128 = iota((QB, 128), 1).astype(F32)

    for t in range(4):
        rows = pl.ds(t * QB, QB)
        sc = cols_ref[rows, :]
        onehot = jnp.concatenate(
            [jnp.where(sc == lane128 + float(128 * b), 1.0, 0.0).astype(BF16) for b in range(8)],
            axis=1,
        )
        x = mm(onehot, raw_ref[...])
        gath_ref[rows, :] = x.astype(BF16)
        centred = x - jnp.mean(x, axis=1, keepdims=True)
        inv = lax.rsqrt(jnp.mean(centred * centred, axis=1, keepdims=True) + EPS)
        normed = centred * inv
        normed_ref[rows, :] = normed
        inv_ref[rows, :] = inv
        hid = (normed * gain).astype(BF16)
        hid_ref[rows, :] = hid
        packed = mm(hid, wqkv_ref[...]).astype(BF16)
        pT_ref[:, rows] = jnp.transpose(packed)
        bp = mm_nt(og_ref[rows, :], wproj_ref[...]).astype(BF16)
        bpT = jnp.transpose(bp)
        lane = iota((C, QB), 1) + t * QB
        doT_ref[:, rows] = jnp.where(lane < n_live, bpT.astype(F32), 0.0).astype(BF16)
        kv_ref[rows, :] = packed[:, C:]

    chan = iota((C, C), 0)
    place = iota((C, C), 1)
    spot = place % 64
    for b in range(4):
        cols = pl.ds(b * C, C)
        same = ((place // 64 + 4 * b) == chan // HD) & (spot % HD == chan % HD)
        rep_k = jnp.where(same & (spot < 3 * HD), 1.0, 0.0).astype(BF16)
        rep_v = jnp.where(same & (spot < 2 * HD), 1.0, 0.0).astype(BF16)
        spot_r = iota((1, C), 1) % 64
        ones_k = jnp.where((spot_r >= 48) & (spot_r < 51), 1.0, 0.0)
        ones_v = jnp.where((spot_r >= 32) & (spot_r < 35), 1.0, 0.0)
        dead_k = jnp.where(spot_r == 51, NEG, 0.0)
        for t in range(4):
            rows = pl.ds(t * QB, QB)
            dead = jnp.where((iota((QB, 1), 0) + t * QB) < n_live, 0.0, 1.0)
            ka = mm(kv_ref[rows, :C], rep_k) + ones_k + dead * dead_k
            ka_ref[rows, cols] = ka.astype(BF16)
            va = mm(kv_ref[rows, C:], rep_v) + ones_v
            va_ref[rows, cols] = va.astype(BF16)

    def prep(h, carry):
        q = pT_ref[pl.ds(h * HD, HD), :].astype(F32)
        k = pT_ref[pl.ds(C + h * HD, HD), :].astype(F32)
        v = pT_ref[pl.ds(2 * C + h * HD, HD), :]
        do = doT_ref[pl.ds(h * HD, HD), :]
        q = q * QSCALE
        hi, mid, lo = split3(q)
        row = iota((HD, N), 0)
        tail = jnp.where(row == 3, 1.0, 0.0).astype(BF16)
        zeros = jnp.zeros((64, N), BF16)
        base = pl.multiple_of(h * 128, 128)
        half = pl.multiple_of((h % 2) * 64, 64)
        qa_ref[pl.ds(pl.multiple_of(base + half, 64), 64), :] = jnp.concatenate(
            [hi, mid, lo, tail], axis=0
        )
        qa_ref[pl.ds(pl.multiple_of(base + 64 - half, 64), 64), :] = zeros
        ones = jnp.where(row == 0, 1.0, 0.0).astype(BF16)
        vt_ref[pl.ds(h * 32, 32), :] = jnp.concatenate([v, ones], axis=0)
        q2 = jnp.max(jnp.sum(q * q, axis=0, keepdims=True))
        k2 = jnp.max(jnp.sum(k * k, axis=0, keepdims=True))
        vmax = jnp.max(jnp.abs(v.astype(F32)))
        dmax = jnp.max(jnp.abs(do.astype(F32)))
        tame = (q2 * k2 <= 8100.0) & (vmax <= 4096.0) & (dmax <= 4096.0)

        @pl.when(jnp.logical_not(tame))
        def _():
            lanes = pl.ds(pl.multiple_of((h // 2) * 128, 128), 128)
            for t in range(NQ):
                cols = pl.ds(t * QB, QB)
                peak = jnp.full((1, QB), -jnp.inf, F32)
                for r in range(4):
                    s = mm(ka_ref[pl.ds(r * QB, QB), lanes], qa_ref[pl.ds(base, 128), cols])
                    peak = jnp.maximum(peak, jnp.max(s, axis=0, keepdims=True))
                p_hi, p_mid, p_lo = split3(-peak)
                rowq = iota((HD, QB), 0)
                shift = jnp.where(rowq == 0, p_hi.astype(F32), 0.0)
                shift = jnp.where(rowq == 1, p_mid.astype(F32), shift)
                shift = jnp.where(rowq == 2, p_lo.astype(F32), shift)
                shift = jnp.where(rowq == 3, 1.0, shift)
                at = pl.multiple_of(base + half + 48, 16)
                qa_ref[pl.ds(at, HD), cols] = shift.astype(BF16)

        return carry

    lax.fori_loop(0, H, prep, 0)

    def names(p, j):
        side, t, slot = j // NA, j % NA, j % 2
        h = 2 * p + side
        hrows = pl.ds(pl.multiple_of(h * HD, HD), HD)
        krows = pl.ds(pl.multiple_of(C + h * HD, HD), HD)
        vrows = pl.ds(pl.multiple_of(2 * C + h * HD, HD), HD)
        lanes = pl.ds(pl.multiple_of(p * 128, 128), 128)
        return side, t, slot, h, slice(t * AQ, (t + 1) * AQ), lanes, hrows, krows, vrows

    def first_stage(p, j):
        side, t, slot, h, cols, lanes, hrows, krows, vrows = names(p, j)
        rhs = qa_ref[pl.ds(pl.multiple_of(h * 128, 128), 128), cols]
        s = mm(ka_ref[:, lanes], rhs)
        e_ref[slot] = jnp.exp2(s).astype(BF16)

    def outputs(p, j):
        side, t, slot, h, cols, lanes, hrows, krows, vrows = names(p, j)
        return mm(vt_ref[pl.ds(pl.multiple_of(h * 32, 32), 32), :], e_ref[slot])

    def cotangents(p, j, o_un):
        side, t, slot, h, cols, lanes, hrows, krows, vrows = names(p, j)
        l_inv = 1.0 / o_un[HD : HD + 1, :]
        o = o_un[:HD, :] * l_inv
        live = (iota((HD, AQ), 1) + t * AQ) < n_live
        attT_ref[hrows, cols] = jnp.where(live, o, 0.0).astype(BF16)
        do = doT_ref[hrows, cols].astype(F32)
        dl = do * l_inv
        d_hi = dl.astype(BF16)
        d_lo = (dl - d_hi.astype(F32)).astype(BF16)
        cross = -jnp.sum(dl * o, axis=0, keepdims=True)
        c_hi, c_mid, c_lo = split3(cross)
        row = iota((32, AQ), 0)
        tail = jnp.where(row == 0, c_hi.astype(F32), 0.0)
        tail = jnp.where(row == 1, c_mid.astype(F32), tail)
        tail = jnp.where(row == 2, c_lo.astype(F32), tail)
        both = jnp.concatenate([d_hi, d_lo], axis=0)
        zeros = jnp.zeros((64, AQ), BF16)
        parts = [both, tail.astype(BF16)]
        parts = parts + [zeros] if side == 0 else [zeros] + parts
        dp = mm(va_ref[:, lanes], jnp.concatenate(parts, axis=0))
        ds_ref[slot] = (e_ref[slot].astype(F32) * dp).astype(BF16)
        return both

    def value_grad(p, j, both):
        side, t, slot, h, cols, lanes, hrows, krows, vrows = names(p, j)
        dv = mm_nt(both, e_ref[slot])
        dv = dv[:HD] + dv[HD:]
        if t > 0:
            dv = dv_ref[...] + dv
        if t < NA - 1:
            dv_ref[...] = dv
        else:
            gpT_ref[vrows, :] = dv.astype(BF16)

    def score_grads(p, j):
        side, t, slot, h, cols, lanes, hrows, krows, vrows = names(p, j)
        dq = mm(pT_ref[krows, :], ds_ref[slot])
        gpT_ref[hrows, cols] = (dq * SCALE).astype(BF16)
        dk = mm_nt(pT_ref[hrows, cols], ds_ref[slot])
        if t > 0:
            dk = dk_ref[...] + dk
        if t < NA - 1:
            dk_ref[...] = dk
        else:
            gpT_ref[krows, :] = (dk * SCALE).astype(BF16)

    first_stage(0, 0)
    if LAG:
        ds_ref[1] = jnp.zeros((N, AQ), BF16)
        dk_ref[...] = jnp.zeros((HD, N), F32)

    def pair(p, carry):
        for j in range(2 * NA):
            o_un = outputs(p, j)
            if j < 2 * NA - 1:
                first_stage(p, j + 1)
            else:
                first_stage(jnp.minimum(p + 1, H // 2 - 1), 0)
            both = cotangents(p, j, o_un)
            if LAG:
                if j > 0:
                    score_grads(p, j - 1)
                else:
                    score_grads(jnp.maximum(p - 1, 0), 2 * NA - 1)
                value_grad(p, j, both)
            else:
                value_grad(p, j, both)
                score_grads(p, j)
        return carry

    lax.fori_loop(0, H // 2, pair, 0)
    if LAG:
        score_grads(H // 2 - 1, 2 * NA - 1)

    grad_ref[: 3 * C, :] = mm(gpT_ref[...], hid_ref[...]) * POINT_SCALE
    grad_ref[3 * C :, :] = mm(attT_ref[...], og_ref[...]) * POINT_SCALE
    for half in range(2):
        part = grad_ref[:, half * 128 : (half + 1) * 128].reshape(128, 8, 128)
        send_ref[:, half * 8 : (half + 1) * 8, :] = part.astype(BF16)

    gain_sum = jnp.zeros((1, C), F32)
    for t in range(4):
        rows = pl.ds(t * QB, QB)
        att = jnp.transpose(attT_ref[:, rows])
        bo = gath_ref[rows, :].astype(F32) + mm(att, wproj_ref[...])
        bo_ref[pl.ds(t * QB + 8, QB), :] = bo.astype(BF16).astype(F32)
        gp = jnp.transpose(gpT_ref[:, rows])
        gh = mm_nt(gp, wqkv_ref[...])
        normed = normed_ref[rows, :]
        gain_sum = gain_sum + jnp.sum(gh * normed, axis=0, keepdims=True)
        g = gh * gain
        mean_g = jnp.mean(g, axis=1, keepdims=True)
        mean_c = jnp.mean(g * normed, axis=1, keepdims=True)
        dx = og_ref[rows, :].astype(F32) + inv_ref[rows, :] * (g - mean_g - normed * mean_c)
        dx_ref[rows, :] = dx.astype(BF16)
    gain_sum = gain_sum * POINT_SCALE
    gsum_ref[0] = gain_sum[:, :128]
    gsum_ref[1] = gain_sum[:, 128:]
    for t in range(4):
        spot = iota((QB, N), 0) + t * QB
        onehot = jnp.where(spot == serial_row, 1.0, 0.0).astype(BF16)
        gfeats_ref[pl.ds(t * QB, QB), :] = mm(onehot, dx_ref[...]).astype(BF16)

    ids_ref[8 : N + 8, :] = jnp.transpose(
        jnp.broadcast_to(cluster_ref[...].astype(F32), (128, N))
    )
    ids_ref[:8, :] = jnp.full((8, 128), -1.0, F32)
    ids_ref[N + 8 :, :] = jnp.full((8, 128), -2.0, F32)
    bo_ref[:8, :] = jnp.full((8, C), -jnp.inf, F32)
    bo_ref[N + 8 :, :] = jnp.full((8, C), -jnp.inf, F32)
    span = 128
    wide = span + 16

    def pool(i, carry):
        at = pl.multiple_of(i * span, span)
        ids = ids_ref[pl.ds(at, wide), :]
        for half in range(2):
            cols = slice(half * 128, (half + 1) * 128)
            m = bo_ref[pl.ds(at, wide), cols]
            for step in (1, 2, 4):
                ok = pltpu.roll(ids, step, 0) == ids
                m = jnp.maximum(m, jnp.where(ok, pltpu.roll(m, step, 0), -jnp.inf))
            for step in (1, 2, 4):
                ok = pltpu.roll(ids, wide - step, 0) == ids
                m = jnp.maximum(m, jnp.where(ok, pltpu.roll(m, wide - step, 0), -jnp.inf))
            bo2_ref[pl.ds(at, span), cols] = m[8 : span + 8]
        return carry

    lax.fori_loop(0, N // span, pool, 0)
    pooled_ref[...] = bo2_ref[...].astype(BF16)
    edge_ref[0, :8, :] = bo2_ref[:8, :]
    edge_ref[1, :8, :] = bo2_ref[N - 8 :, :]
    flag = jnp.full((8, C), joined_ref[0], jnp.int32).astype(F32)
    edge_ref[0, 8:, :] = flag
    edge_ref[1, 8:, :] = flag


def local_part(raw, serial, counts, gain, w_qkv, w_proj, out_grad, cluster, joined):
    shapes = (
        jax.ShapeDtypeStruct((N, C), BF16),
        jax.ShapeDtypeStruct((N, C), BF16),
        jax.ShapeDtypeStruct((128, 16, 128), BF16),
        jax.ShapeDtypeStruct((2, 1, 128), F32),
        jax.ShapeDtypeStruct((2, 16, C), F32),
    )
    vm = pl.BlockSpec(memory_space=VMEM)
    sm = pl.BlockSpec(memory_space=pltpu.SMEM)
    return pl.pallas_call(
        local_kernel,
        out_shape=shapes,
        in_specs=[vm, vm, sm, vm, vm, vm, vm, vm, sm],
        out_specs=[vm] * 5,
        scratch_shapes=[
            VMEM((N, C), BF16),
            VMEM((N, C), BF16),
            VMEM((N, C), F32),
            VMEM((N, 1), F32),
            VMEM((3 * C, N), BF16),
            VMEM((C, N), BF16),
            VMEM((N, 4 * C), BF16),
            VMEM((N, 4 * C), BF16),
            VMEM((H * 128, N), BF16),
            VMEM((H * 32, N), BF16),
            VMEM((2, N, AQ), BF16),
            VMEM((2, N, AQ), BF16),
            VMEM((C, N), BF16),
            VMEM((3 * C, N), BF16),
            VMEM((HD, N), F32),
            VMEM((HD, N), F32),
            VMEM((N, C), F32),
            VMEM((N, C), BF16),
            VMEM((N + 16, C), F32),
            VMEM((N, C), F32),
            VMEM((N + 16, 128), F32),
            VMEM((N, 128), F32),
            VMEM((N, 2 * C), BF16),
        ],
        compiler_params=pltpu.CompilerParams(vmem_limit_bytes=56 * 1024 * 1024),
        name="local_part",
    )(raw, serial, counts, gain, w_qkv, w_proj, out_grad, cluster, joined)


def comm_kernel(
    send_ref,
    gsum_ref,
    edge_ref,
    ends_in_ref,
    cluster_ref,
    ends_ref,
    gqkv_ref,
    gproj_ref,
    ggain_ref,
    pair_buf,
    pair_gain,
    edge_buf,
    chip_buf,
    chip_gain,
    rs_buf,
    gain_buf,
    ag_buf,
    out_buf,
    gain_out,
    grad_buf,
    sems,
):
    y = lax.axis_index("order_0")
    x = lax.axis_index("order_1")
    core = lax.axis_index("order_2")
    z = lax.axis_index("help")
    chip = (y * 4 + x) * 4 + z
    shard = ((y * 4 + x) * 2 + core) * 4 + z

    def of_shard(s):
        return (s // 32, (s // 8) % 4, (s // 4) % 2, s % 4)

    def of_chip(r):
        return ((y + r // 16) % 4, (x + (r // 4) % 4) % 4, core, (z + r % 4) % 4)

    partner = (y, x, 1 - core, z)
    following = of_shard((shard + 1) % 128)
    previous = of_shard((shard + 127) % 128)

    barrier = pltpu.get_barrier_semaphore()

    def greet(r, carry):
        pl.semaphore_signal(barrier, inc=1, device_id=of_chip(r), device_id_type=MESH)
        return carry

    lax.fori_loop(1, 64, greet, 0)
    for other in (partner, following, previous):
        pl.semaphore_signal(barrier, inc=1, device_id=other, device_id_type=MESH)
    pl.semaphore_wait(barrier, 66)

    def remote(src, dst, i, device):
        return pltpu.make_async_remote_copy(
            src_ref=src,
            dst_ref=dst,
            send_sem=sems.at[2 * i],
            recv_sem=sems.at[2 * i + 1],
            device_id=device,
            device_id_type=MESH,
        )

    far = 64 * (1 - core)
    pair_copy = remote(send_ref.at[pl.ds(far, 64)], pair_buf, 0, partner)
    pair_copy.start()
    pair_gain_copy = remote(gsum_ref.at[1 - core], pair_gain, 1, partner)
    pair_gain_copy.start()
    ahead = remote(edge_ref.at[1], edge_buf.at[0], 2, following)
    ahead.start()
    back = remote(edge_ref.at[0], edge_buf.at[1], 3, previous)
    back.start()

    pair_copy.wait()
    mine = send_ref[pl.ds(64 * core, 64)].astype(F32) + pair_buf[...].astype(F32)
    chip_buf[...] = mine.astype(BF16)
    pair_gain_copy.wait()
    chip_gain[...] = gsum_ref[core] + pair_gain[...]

    def scatter(r, carry):
        to = of_chip(r)
        other = (to[0] * 4 + to[1]) * 4 + to[3]
        remote(chip_buf.at[other], rs_buf.at[chip], 4, to).start()
        remote(chip_gain, gain_buf.at[chip], 5, to).start()
        return carry

    lax.fori_loop(1, 64, scatter, 0)
    rs_buf[pl.ds(chip, 1)] = chip_buf[pl.ds(chip, 1)]
    gain_buf[pl.ds(chip, 1)] = chip_gain[...][None]

    ahead.wait()
    back.wait()
    ids = jnp.transpose(jnp.broadcast_to(cluster_ref[...].astype(F32), (128, N)))
    first = ids[:8]
    last = ids[N - 8 :]
    linked = (edge_ref[0, 8:9, :128] > 0.0) & (shard > 0)
    head_ok = (first == first[:1]) & linked
    next_joined = edge_buf[1, 8:9, :128] > 0.0
    tail_ok = (last == last[7:8]) & next_joined & (shard < 127)
    for half in range(2):
        cols = slice(half * 128, (half + 1) * 128)
        from_prev = edge_buf[0, 7:8, cols]
        from_next = edge_buf[1, 0:1, cols]
        top = edge_ref[0, 0:8, cols]
        top = jnp.where(head_ok, jnp.maximum(top, from_prev), top)
        low = edge_ref[1, 0:8, cols]
        low = jnp.where(tail_ok, jnp.maximum(low, from_next), low)
        above = ends_in_ref[8:16, cols].astype(F32)
        below = ends_in_ref[16:24, cols].astype(F32)
        ends_ref[:16, cols] = jnp.concatenate([top, above], axis=0).astype(BF16)
        ends_ref[16:, cols] = jnp.concatenate([below, low], axis=0).astype(BF16)

    everything = pl.ds(0, 63)
    for i, (src, dst) in ((4, (ag_buf, rs_buf)), (5, (gain_out, gain_buf))):
        whole = remote(dst.at[everything], dst.at[everything], i, partner)
        whole.wait_recv()
        whole.wait_send()
    total = jnp.sum(rs_buf[...].astype(F32), axis=0)
    ag_buf[pl.ds(chip, 1)] = total.astype(BF16)[None]

    def gather(r, carry):
        remote(ag_buf.at[chip], ag_buf.at[chip], 6, of_chip(r)).start()
        return carry

    lax.fori_loop(1, 64, gather, 0)
    gain_out[pl.ds(core, 1)] = jnp.sum(gain_buf[...], axis=0)[None]
    last_gain = remote(gain_out.at[core], gain_out.at[core], 7, partner)
    last_gain.start()
    whole = remote(ag_buf.at[everything], ag_buf.at[everything], 6, partner)
    whole.wait_recv()
    whole.wait_send()
    last_copy = remote(ag_buf, out_buf.at[core], 8, partner)
    last_copy.start()
    out_buf[pl.ds(core, 1)] = ag_buf[...][None]
    last_gain.wait()
    ggain_ref[:, :128] = gain_out[0]
    ggain_ref[:, 128:] = gain_out[1]
    last_copy.wait()
    for c in range(2):
        for half in range(2):
            part = out_buf[c, :, half * 8 : (half + 1) * 8, :].astype(F32).reshape(512, 128)
            grad_buf[c * 512 : (c + 1) * 512, half * 128 : (half + 1) * 128] = part
    gqkv_ref[...] = jnp.transpose(grad_buf[: 3 * C, :])
    gproj_ref[...] = grad_buf[3 * C :, :]


def comm_part(send, gsum, edge, ends, cluster):
    shapes = (
        jax.ShapeDtypeStruct((32, C), BF16),
        jax.ShapeDtypeStruct((C, 3 * C), F32),
        jax.ShapeDtypeStruct((C, C), F32),
        jax.ShapeDtypeStruct((1, C), F32),
    )
    vm = pl.BlockSpec(memory_space=VMEM)
    return pl.pallas_call(
        comm_kernel,
        out_shape=shapes,
        in_specs=[vm] * 5,
        out_specs=[vm] * 4,
        scratch_shapes=[
            VMEM((64, 16, 128), BF16),
            VMEM((1, 128), F32),
            VMEM((2, 16, C), F32),
            VMEM((64, 16, 128), BF16),
            VMEM((1, 128), F32),
            VMEM((64, 16, 128), BF16),
            VMEM((64, 1, 128), F32),
            VMEM((64, 16, 128), BF16),
            VMEM((2, 64, 16, 128), BF16),
            VMEM((2, 1, 128), F32),
            VMEM((N, C), F32),
            pltpu.SemaphoreType.DMA((18,)),
        ],
        compiler_params=pltpu.CompilerParams(
            collective_id=0, has_side_effects=True, vmem_limit_bytes=32 * 1024 * 1024
        ),
        name="comm_part",
    )(send, gsum, edge, ends, cluster)


def body(raw_feats, serial, counts, norm_gain, w_qkv, w_proj, out_grad, cluster, joined):
    pooled, grad_feats, send, gsum, edge = local_part(
        raw_feats[0], serial, counts, norm_gain[None], w_qkv, w_proj, out_grad[0], cluster, joined
    )
    ends = jnp.concatenate([pooled[:16], pooled[N - 16 :]], axis=0)
    ends, grad_qkv, grad_proj, grad_gain = comm_part(send, gsum, edge, ends, cluster)
    pooled = pooled.at[:16].set(ends[:16]).at[N - 16 :].set(ends[16:])
    return (pooled[None], grad_feats[None], grad_qkv, grad_proj, grad_gain[0])


def solution(mesh):
    torus = Mesh(
        mesh.devices.reshape(4, 4, 2, mesh.shape["help"]), ("order_0", "order_1", "order_2", "help")
    )
    placed = (
        P(ORDER_HELP, None, None),
        P(ORDER_HELP, None),
        P(ORDER_HELP, None),
        P(),
        P(),
        P(),
        P(ORDER_HELP, None, None),
        P(ORDER_HELP, None),
        P(ORDER_HELP),
    )
    return jax.shard_map(
        body,
        mesh=torus,
        in_specs=placed,
        out_specs=(P(ORDER_HELP, None, None), P(ORDER_HELP, None, None), P(), P(), P()),
        check_vma=False,
    )
```

```python
import math

import jax
import jax.numpy as jnp
from jax import lax
from jax.experimental import pallas as pl
from jax.experimental.pallas import tpu as pltpu
from jax.sharding import Mesh
from jax.sharding import PartitionSpec as P

H = 16
C = 256
N = 1024
HD = 16
QB = 256
NQ = N // QB
AQ = 512
NA = N // AQ
LAG = False
GROUP = 8
ORDER_HELP = ("order_0", "order_1", "order_2", "help")
EPS = 1e-05
NEG = -1e30
SCALE = HD**-0.5
QSCALE = SCALE * math.log2(math.e)
POINT_SCALE = 2.0 * N**-0.5
F32 = jnp.float32
BF16 = jnp.bfloat16
MESH = pl.DeviceIdType.MESH
VMEM = pltpu.VMEM


def iota(shape, dim):
    return lax.broadcasted_iota(jnp.int32, shape, dim)


def mm(a, b):
    return jnp.dot(a, b, preferred_element_type=F32)


def mm_nt(a, b):
    return lax.dot_general(a, b, (((1,), (1,)), ((), ())), preferred_element_type=F32)


def split3(x):
    hi = x.astype(BF16)
    rest = x - hi.astype(F32)
    mid = rest.astype(BF16)
    lo = (rest - mid.astype(F32)).astype(BF16)
    return hi, mid, lo


def local_kernel(
    raw_ref,
    serial_ref,
    counts_ref,
    gain_ref,
    wqkv_ref,
    wproj_ref,
    og_ref,
    cluster_ref,
    joined_ref,
    pooled_ref,
    gfeats_ref,
    send_ref,
    gsum_ref,
    edge_ref,
    gath_ref,
    hid_ref,
    normed_ref,
    inv_ref,
    pT_ref,
    doT_ref,
    ka_ref,
    va_ref,
    qa_ref,
    vt_ref,
    e_ref,
    ds_ref,
    attT_ref,
    gpT_ref,
    dk_ref,
    dv_ref,
    grad_ref,
    dx_ref,
    bo_ref,
    bo2_ref,
    ids_ref,
    cols_ref,
    kv_ref,
    et_ref,
    dst_ref,
):
    n_live = counts_ref[0, 0]
    gain = gain_ref[...]
    serial_row = serial_ref[...]
    cols_ref[...] = jnp.transpose(jnp.broadcast_to(serial_row.astype(F32), (128, N)))
    lane128 = iota((QB, 128), 1).astype(F32)

    for t in range(4):
        rows = pl.ds(t * QB, QB)
        sc = cols_ref[rows, :]
        onehot = jnp.concatenate(
            [jnp.where(sc == lane128 + float(128 * b), 1.0, 0.0).astype(BF16) for b in range(8)],
            axis=1,
        )
        x = mm(onehot, raw_ref[...])
        gath_ref[rows, :] = x.astype(BF16)
        centred = x - jnp.mean(x, axis=1, keepdims=True)
        inv = lax.rsqrt(jnp.mean(centred * centred, axis=1, keepdims=True) + EPS)
        normed = centred * inv
        normed_ref[rows, :] = normed
        inv_ref[rows, :] = inv
        hid = (normed * gain).astype(BF16)
        hid_ref[rows, :] = hid
        packed = mm(hid, wqkv_ref[...]).astype(BF16)
        pT_ref[:, rows] = jnp.transpose(packed)
        bp = mm_nt(og_ref[rows, :], wproj_ref[...]).astype(BF16)
        bpT = jnp.transpose(bp)
        lane = iota((C, QB), 1) + t * QB
        doT_ref[:, rows] = jnp.where(lane < n_live, bpT.astype(F32), 0.0).astype(BF16)
        kv_ref[rows, :] = packed[:, C:]

    chan = iota((C, C), 0)
    place = iota((C, C), 1)
    spot = place % 64
    for b in range(4):
        cols = pl.ds(b * C, C)
        same = ((place // 64 + 4 * b) == chan // HD) & (spot % HD == chan % HD)
        rep_k = jnp.where(same & (spot < 3 * HD), 1.0, 0.0).astype(BF16)
        rep_v = jnp.where(same & (spot < 2 * HD), 1.0, 0.0).astype(BF16)
        spot_r = iota((1, C), 1) % 64
        ones_k = jnp.where((spot_r >= 48) & (spot_r < 51), 1.0, 0.0)
        ones_v = jnp.where((spot_r >= 32) & (spot_r < 35), 1.0, 0.0)
        dead_k = jnp.where(spot_r == 51, NEG, 0.0)
        for t in range(4):
            rows = pl.ds(t * QB, QB)
            dead = jnp.where((iota((QB, 1), 0) + t * QB) < n_live, 0.0, 1.0)
            ka = mm(kv_ref[rows, :C], rep_k) + ones_k + dead * dead_k
            ka_ref[rows, cols] = ka.astype(BF16)
            va = mm(kv_ref[rows, C:], rep_v) + ones_v
            va_ref[rows, cols] = va.astype(BF16)

    def prep(h, carry):
        q = pT_ref[pl.ds(h * HD, HD), :].astype(F32)
        k = pT_ref[pl.ds(C + h * HD, HD), :].astype(F32)
        v = pT_ref[pl.ds(2 * C + h * HD, HD), :]
        do = doT_ref[pl.ds(h * HD, HD), :]
        q = q * QSCALE
        hi, mid, lo = split3(q)
        row = iota((HD, N), 0)
        tail = jnp.where(row == 3, 1.0, 0.0).astype(BF16)
        zeros = jnp.zeros((64, N), BF16)
        base = pl.multiple_of(h * 128, 128)
        half = pl.multiple_of((h % 2) * 64, 64)
        qa_ref[pl.ds(pl.multiple_of(base + half, 64), 64), :] = jnp.concatenate(
            [hi, mid, lo, tail], axis=0
        )
        qa_ref[pl.ds(pl.multiple_of(base + 64 - half, 64), 64), :] = zeros
        ones = jnp.where(row == 0, 1.0, 0.0).astype(BF16)
        vt_ref[pl.ds(h * 32, 32), :] = jnp.concatenate([v, ones], axis=0)
        q2 = jnp.max(jnp.sum(q * q, axis=0, keepdims=True))
        k2 = jnp.max(jnp.sum(k * k, axis=0, keepdims=True))
        vmax = jnp.max(jnp.abs(v.astype(F32)))
        dmax = jnp.max(jnp.abs(do.astype(F32)))
        tame = (q2 * k2 <= 8100.0) & (vmax <= 4096.0) & (dmax <= 4096.0)

        @pl.when(jnp.logical_not(tame))
        def _():
            lanes = pl.ds(pl.multiple_of((h // 2) * 128, 128), 128)
            for t in range(NQ):
                cols = pl.ds(t * QB, QB)
                peak = jnp.full((1, QB), -jnp.inf, F32)
                for r in range(4):
                    s = mm(ka_ref[pl.ds(r * QB, QB), lanes], qa_ref[pl.ds(base, 128), cols])
                    peak = jnp.maximum(peak, jnp.max(s, axis=0, keepdims=True))
                p_hi, p_mid, p_lo = split3(-peak)
                rowq = iota((HD, QB), 0)
                shift = jnp.where(rowq == 0, p_hi.astype(F32), 0.0)
                shift = jnp.where(rowq == 1, p_mid.astype(F32), shift)
                shift = jnp.where(rowq == 2, p_lo.astype(F32), shift)
                shift = jnp.where(rowq == 3, 1.0, shift)
                at = pl.multiple_of(base + half + 48, 16)
                qa_ref[pl.ds(at, HD), cols] = shift.astype(BF16)

        return carry

    lax.fori_loop(0, H, prep, 0)

    def names(p, j):
        side, t, slot = j // NA, j % NA, j % 2
        h = 2 * p + side
        hrows = pl.ds(pl.multiple_of(h * HD, HD), HD)
        krows = pl.ds(pl.multiple_of(C + h * HD, HD), HD)
        vrows = pl.ds(pl.multiple_of(2 * C + h * HD, HD), HD)
        lanes = pl.ds(pl.multiple_of(p * 128, 128), 128)
        return side, t, slot, h, slice(t * AQ, (t + 1) * AQ), lanes, hrows, krows, vrows

    def first_stage(p, j):
        side, t, slot, h, cols, lanes, hrows, krows, vrows = names(p, j)
        rhs = qa_ref[pl.ds(pl.multiple_of(h * 128, 128), 128), cols]
        s = mm(ka_ref[:, lanes], rhs)
        e = jnp.exp2(s).astype(BF16)
        e_ref[slot] = e
        et_ref[slot] = jnp.transpose(e)

    def outputs(p, j):
        side, t, slot, h, cols, lanes, hrows, krows, vrows = names(p, j)
        return mm(vt_ref[pl.ds(pl.multiple_of(h * 32, 32), 32), :], e_ref[slot])

    def cotangents(p, j, o_un):
        side, t, slot, h, cols, lanes, hrows, krows, vrows = names(p, j)
        l_inv = 1.0 / o_un[HD : HD + 1, :]
        o = o_un[:HD, :] * l_inv
        live = (iota((HD, AQ), 1) + t * AQ) < n_live
        attT_ref[hrows, cols] = jnp.where(live, o, 0.0).astype(BF16)
        do = doT_ref[hrows, cols].astype(F32)
        dl = do * l_inv
        d_hi = dl.astype(BF16)
        d_lo = (dl - d_hi.astype(F32)).astype(BF16)
        cross = -jnp.sum(dl * o, axis=0, keepdims=True)
        c_hi, c_mid, c_lo = split3(cross)
        row = iota((32, AQ), 0)
        tail = jnp.where(row == 0, c_hi.astype(F32), 0.0)
        tail = jnp.where(row == 1, c_mid.astype(F32), tail)
        tail = jnp.where(row == 2, c_lo.astype(F32), tail)
        both = jnp.concatenate([d_hi, d_lo], axis=0)
        zeros = jnp.zeros((64, AQ), BF16)
        parts = [both, tail.astype(BF16)]
        parts = parts + [zeros] if side == 0 else [zeros] + parts
        dp = mm(va_ref[:, lanes], jnp.concatenate(parts, axis=0))
        ds = (e_ref[slot].astype(F32) * dp).astype(BF16)
        ds_ref[slot] = ds
        dst_ref[slot] = jnp.transpose(ds)
        return both

    def value_grad(p, j, both):
        side, t, slot, h, cols, lanes, hrows, krows, vrows = names(p, j)
        dv = mm(both, et_ref[slot])
        dv = dv[:HD] + dv[HD:]
        if t > 0:
            dv = dv_ref[...] + dv
        if t < NA - 1:
            dv_ref[...] = dv
        else:
            gpT_ref[vrows, :] = dv.astype(BF16)

    def score_grads(p, j):
        side, t, slot, h, cols, lanes, hrows, krows, vrows = names(p, j)
        dq = mm(pT_ref[krows, :], ds_ref[slot])
        gpT_ref[hrows, cols] = (dq * SCALE).astype(BF16)
        dk = mm(pT_ref[hrows, cols], dst_ref[slot])
        if t > 0:
            dk = dk_ref[...] + dk
        if t < NA - 1:
            dk_ref[...] = dk
        else:
            gpT_ref[krows, :] = (dk * SCALE).astype(BF16)

    first_stage(0, 0)
    if LAG:
        ds_ref[1] = jnp.zeros((N, AQ), BF16)
        dst_ref[1] = jnp.zeros((AQ, N), BF16)
        dk_ref[...] = jnp.zeros((HD, N), F32)

    def pair(p, carry):
        for j in range(2 * NA):
            o_un = outputs(p, j)
            if j < 2 * NA - 1:
                first_stage(p, j + 1)
            else:
                first_stage(jnp.minimum(p + 1, H // 2 - 1), 0)
            both = cotangents(p, j, o_un)
            if LAG:
                if j > 0:
                    score_grads(p, j - 1)
                else:
                    score_grads(jnp.maximum(p - 1, 0), 2 * NA - 1)
                value_grad(p, j, both)
            else:
                value_grad(p, j, both)
                score_grads(p, j)
        return carry

    lax.fori_loop(0, H // 2, pair, 0)
    if LAG:
        score_grads(H // 2 - 1, 2 * NA - 1)

    grad_ref[: 3 * C, :] = mm(gpT_ref[...], hid_ref[...]) * POINT_SCALE
    grad_ref[3 * C :, :] = mm(attT_ref[...], og_ref[...]) * POINT_SCALE
    for half in range(2):
        part = grad_ref[:, half * 128 : (half + 1) * 128].reshape(128, 8, 128)
        send_ref[:, half * 8 : (half + 1) * 8, :] = part.astype(BF16)

    gain_sum = jnp.zeros((1, C), F32)
    for t in range(4):
        rows = pl.ds(t * QB, QB)
        att = jnp.transpose(attT_ref[:, rows])
        bo = gath_ref[rows, :].astype(F32) + mm(att, wproj_ref[...])
        bo_ref[pl.ds(t * QB + 8, QB), :] = bo.astype(BF16).astype(F32)
        gp = jnp.transpose(gpT_ref[:, rows])
        gh = mm_nt(gp, wqkv_ref[...])
        normed = normed_ref[rows, :]
        gain_sum = gain_sum + jnp.sum(gh * normed, axis=0, keepdims=True)
        g = gh * gain
        mean_g = jnp.mean(g, axis=1, keepdims=True)
        mean_c = jnp.mean(g * normed, axis=1, keepdims=True)
        dx = og_ref[rows, :].astype(F32) + inv_ref[rows, :] * (g - mean_g - normed * mean_c)
        dx_ref[rows, :] = dx.astype(BF16)
    gain_sum = gain_sum * POINT_SCALE
    gsum_ref[0] = gain_sum[:, :128]
    gsum_ref[1] = gain_sum[:, 128:]
    for t in range(4):
        spot = iota((QB, N), 0) + t * QB
        onehot = jnp.where(spot == serial_row, 1.0, 0.0).astype(BF16)
        gfeats_ref[pl.ds(t * QB, QB), :] = mm(onehot, dx_ref[...]).astype(BF16)

    ids_ref[8 : N + 8, :] = jnp.transpose(
        jnp.broadcast_to(cluster_ref[...].astype(F32), (128, N))
    )
    ids_ref[:8, :] = jnp.full((8, 128), -1.0, F32)
    ids_ref[N + 8 :, :] = jnp.full((8, 128), -2.0, F32)
    bo_ref[:8, :] = jnp.full((8, C), -jnp.inf, F32)
    bo_ref[N + 8 :, :] = jnp.full((8, C), -jnp.inf, F32)
    span = 128
    wide = span + 16

    def pool(i, carry):
        at = pl.multiple_of(i * span, span)
        ids = ids_ref[pl.ds(at, wide), :]
        for half in range(2):
            cols = slice(half * 128, (half + 1) * 128)
            m = bo_ref[pl.ds(at, wide), cols]
            for step in (1, 2, 4):
                ok = pltpu.roll(ids, step, 0) == ids
                m = jnp.maximum(m, jnp.where(ok, pltpu.roll(m, step, 0), -jnp.inf))
            for step in (1, 2, 4):
                ok = pltpu.roll(ids, wide - step, 0) == ids
                m = jnp.maximum(m, jnp.where(ok, pltpu.roll(m, wide - step, 0), -jnp.inf))
            bo2_ref[pl.ds(at, span), cols] = m[8 : span + 8]
        return carry

    lax.fori_loop(0, N // span, pool, 0)
    pooled_ref[...] = bo2_ref[...].astype(BF16)
    edge_ref[0, :8, :] = bo2_ref[:8, :]
    edge_ref[1, :8, :] = bo2_ref[N - 8 :, :]
    flag = jnp.full((8, C), joined_ref[0], jnp.int32).astype(F32)
    edge_ref[0, 8:, :] = flag
    edge_ref[1, 8:, :] = flag


def local_part(raw, serial, counts, gain, w_qkv, w_proj, out_grad, cluster, joined):
    shapes = (
        jax.ShapeDtypeStruct((N, C), BF16),
        jax.ShapeDtypeStruct((N, C), BF16),
        jax.ShapeDtypeStruct((128, 16, 128), BF16),
        jax.ShapeDtypeStruct((2, 1, 128), F32),
        jax.ShapeDtypeStruct((2, 16, C), F32),
    )
    vm = pl.BlockSpec(memory_space=VMEM)
    sm = pl.BlockSpec(memory_space=pltpu.SMEM)
    return pl.pallas_call(
        local_kernel,
        out_shape=shapes,
        in_specs=[vm, vm, sm, vm, vm, vm, vm, vm, sm],
        out_specs=[vm] * 5,
        scratch_shapes=[
            VMEM((N, C), BF16),
            VMEM((N, C), BF16),
            VMEM((N, C), F32),
            VMEM((N, 1), F32),
            VMEM((3 * C, N), BF16),
            VMEM((C, N), BF16),
            VMEM((N, 4 * C), BF16),
            VMEM((N, 4 * C), BF16),
            VMEM((H * 128, N), BF16),
            VMEM((H * 32, N), BF16),
            VMEM((2, N, AQ), BF16),
            VMEM((2, N, AQ), BF16),
            VMEM((C, N), BF16),
            VMEM((3 * C, N), BF16),
            VMEM((HD, N), F32),
            VMEM((HD, N), F32),
            VMEM((N, C), F32),
            VMEM((N, C), BF16),
            VMEM((N + 16, C), F32),
            VMEM((N, C), F32),
            VMEM((N + 16, 128), F32),
            VMEM((N, 128), F32),
            VMEM((N, 2 * C), BF16),
            VMEM((2, AQ, N), BF16),
            VMEM((2, AQ, N), BF16),
        ],
        compiler_params=pltpu.CompilerParams(vmem_limit_bytes=56 * 1024 * 1024),
        name="local_part",
    )(raw, serial, counts, gain, w_qkv, w_proj, out_grad, cluster, joined)


def comm_kernel(
    send_ref,
    gsum_ref,
    edge_ref,
    ends_in_ref,
    cluster_ref,
    ends_ref,
    gqkv_ref,
    gproj_ref,
    ggain_ref,
    pair_buf,
    pair_gain,
    edge_buf,
    chip_buf,
    chip_gain,
    rs_buf,
    gain_buf,
    ag_buf,
    out_buf,
    gain_out,
    grad_buf,
    sems,
):
    y = lax.axis_index("order_0")
    x = lax.axis_index("order_1")
    core = lax.axis_index("order_2")
    z = lax.axis_index("help")
    chip = (y * 4 + x) * 4 + z
    shard = ((y * 4 + x) * 2 + core) * 4 + z

    def of_shard(s):
        return (s // 32, (s // 8) % 4, (s // 4) % 2, s % 4)

    def of_chip(r):
        return ((y + r // 16) % 4, (x + (r // 4) % 4) % 4, core, (z + r % 4) % 4)

    partner = (y, x, 1 - core, z)
    following = of_shard((shard + 1) % 128)
    previous = of_shard((shard + 127) % 128)

    barrier = pltpu.get_barrier_semaphore()

    def greet(r, carry):
        pl.semaphore_signal(barrier, inc=1, device_id=of_chip(r), device_id_type=MESH)
        return carry

    lax.fori_loop(1, 64, greet, 0)
    for other in (partner, following, previous):
        pl.semaphore_signal(barrier, inc=1, device_id=other, device_id_type=MESH)
    pl.semaphore_wait(barrier, 66)

    def remote(src, dst, i, device):
        return pltpu.make_async_remote_copy(
            src_ref=src,
            dst_ref=dst,
            send_sem=sems.at[2 * i],
            recv_sem=sems.at[2 * i + 1],
            device_id=device,
            device_id_type=MESH,
        )

    far = 64 * (1 - core)
    pair_copy = remote(send_ref.at[pl.ds(far, 64)], pair_buf, 0, partner)
    pair_copy.start()
    pair_gain_copy = remote(gsum_ref.at[1 - core], pair_gain, 1, partner)
    pair_gain_copy.start()
    ahead = remote(edge_ref.at[1], edge_buf.at[0], 2, following)
    ahead.start()
    back = remote(edge_ref.at[0], edge_buf.at[1], 3, previous)
    back.start()

    pair_copy.wait()
    mine = send_ref[pl.ds(64 * core, 64)].astype(F32) + pair_buf[...].astype(F32)
    chip_buf[...] = mine.astype(BF16)
    pair_gain_copy.wait()
    chip_gain[...] = gsum_ref[core] + pair_gain[...]

    def scatter(r, carry):
        to = of_chip(r)
        other = (to[0] * 4 + to[1]) * 4 + to[3]
        remote(chip_buf.at[other], rs_buf.at[chip], 4, to).start()
        remote(chip_gain, gain_buf.at[chip], 5, to).start()
        return carry

    lax.fori_loop(1, 64, scatter, 0)
    rs_buf[pl.ds(chip, 1)] = chip_buf[pl.ds(chip, 1)]
    gain_buf[pl.ds(chip, 1)] = chip_gain[...][None]

    ahead.wait()
    back.wait()
    ids = jnp.transpose(jnp.broadcast_to(cluster_ref[...].astype(F32), (128, N)))
    first = ids[:8]
    last = ids[N - 8 :]
    linked = (edge_ref[0, 8:9, :128] > 0.0) & (shard > 0)
    head_ok = (first == first[:1]) & linked
    next_joined = edge_buf[1, 8:9, :128] > 0.0
    tail_ok = (last == last[7:8]) & next_joined & (shard < 127)
    for half in range(2):
        cols = slice(half * 128, (half + 1) * 128)
        from_prev = edge_buf[0, 7:8, cols]
        from_next = edge_buf[1, 0:1, cols]
        top = edge_ref[0, 0:8, cols]
        top = jnp.where(head_ok, jnp.maximum(top, from_prev), top)
        low = edge_ref[1, 0:8, cols]
        low = jnp.where(tail_ok, jnp.maximum(low, from_next), low)
        above = ends_in_ref[8:16, cols].astype(F32)
        below = ends_in_ref[16:24, cols].astype(F32)
        ends_ref[:16, cols] = jnp.concatenate([top, above], axis=0).astype(BF16)
        ends_ref[16:, cols] = jnp.concatenate([below, low], axis=0).astype(BF16)

    everything = pl.ds(0, 63)
    for i, (src, dst) in ((4, (ag_buf, rs_buf)), (5, (gain_out, gain_buf))):
        whole = remote(dst.at[everything], dst.at[everything], i, partner)
        whole.wait_recv()
        whole.wait_send()
    total = jnp.sum(rs_buf[...].astype(F32), axis=0)
    ag_buf[pl.ds(chip, 1)] = total.astype(BF16)[None]

    def gather(r, carry):
        remote(ag_buf.at[chip], ag_buf.at[chip], 6, of_chip(r)).start()
        return carry

    lax.fori_loop(1, 64, gather, 0)
    gain_out[pl.ds(core, 1)] = jnp.sum(gain_buf[...], axis=0)[None]
    last_gain = remote(gain_out.at[core], gain_out.at[core], 7, partner)
    last_gain.start()
    whole = remote(ag_buf.at[everything], ag_buf.at[everything], 6, partner)
    whole.wait_recv()
    whole.wait_send()
    last_copy = remote(ag_buf, out_buf.at[core], 8, partner)
    last_copy.start()
    out_buf[pl.ds(core, 1)] = ag_buf[...][None]
    last_gain.wait()
    ggain_ref[:, :128] = gain_out[0]
    ggain_ref[:, 128:] = gain_out[1]
    last_copy.wait()
    for c in range(2):
        for half in range(2):
            part = out_buf[c, :, half * 8 : (half + 1) * 8, :].astype(F32).reshape(512, 128)
            grad_buf[c * 512 : (c + 1) * 512, half * 128 : (half + 1) * 128] = part
    gqkv_ref[...] = jnp.transpose(grad_buf[: 3 * C, :])
    gproj_ref[...] = grad_buf[3 * C :, :]


def comm_part(send, gsum, edge, ends, cluster):
    shapes = (
        jax.ShapeDtypeStruct((32, C), BF16),
        jax.ShapeDtypeStruct((C, 3 * C), F32),
        jax.ShapeDtypeStruct((C, C), F32),
        jax.ShapeDtypeStruct((1, C), F32),
    )
    vm = pl.BlockSpec(memory_space=VMEM)
    return pl.pallas_call(
        comm_kernel,
        out_shape=shapes,
        in_specs=[vm] * 5,
        out_specs=[vm] * 4,
        scratch_shapes=[
            VMEM((64, 16, 128), BF16),
            VMEM((1, 128), F32),
            VMEM((2, 16, C), F32),
            VMEM((64, 16, 128), BF16),
            VMEM((1, 128), F32),
            VMEM((64, 16, 128), BF16),
            VMEM((64, 1, 128), F32),
            VMEM((64, 16, 128), BF16),
            VMEM((2, 64, 16, 128), BF16),
            VMEM((2, 1, 128), F32),
            VMEM((N, C), F32),
            pltpu.SemaphoreType.DMA((18,)),
        ],
        compiler_params=pltpu.CompilerParams(
            collective_id=0, has_side_effects=True, vmem_limit_bytes=32 * 1024 * 1024
        ),
        name="comm_part",
    )(send, gsum, edge, ends, cluster)


def body(raw_feats, serial, counts, norm_gain, w_qkv, w_proj, out_grad, cluster, joined):
    pooled, grad_feats, send, gsum, edge = local_part(
        raw_feats[0], serial, counts, norm_gain[None], w_qkv, w_proj, out_grad[0], cluster, joined
    )
    ends = jnp.concatenate([pooled[:16], pooled[N - 16 :]], axis=0)
    ends, grad_qkv, grad_proj, grad_gain = comm_part(send, gsum, edge, ends, cluster)
    pooled = pooled.at[:16].set(ends[:16]).at[N - 16 :].set(ends[16:])
    return (pooled[None], grad_feats[None], grad_qkv, grad_proj, grad_gain[0])


def solution(mesh):
    torus = Mesh(
        mesh.devices.reshape(4, 4, 2, mesh.shape["help"]), ("order_0", "order_1", "order_2", "help")
    )
    placed = (
        P(ORDER_HELP, None, None),
        P(ORDER_HELP, None),
        P(ORDER_HELP, None),
        P(),
        P(),
        P(),
        P(ORDER_HELP, None, None),
        P(ORDER_HELP, None),
        P(ORDER_HELP),
    )
    return jax.shard_map(
        body,
        mesh=torus,
        in_specs=placed,
        out_specs=(P(ORDER_HELP, None, None), P(ORDER_HELP, None, None), P(), P(), P()),
        check_vma=False,
    )
```

```python
import math

import jax
import jax.numpy as jnp
from jax import lax
from jax.experimental import pallas as pl
from jax.experimental.pallas import tpu as pltpu
from jax.sharding import Mesh
from jax.sharding import PartitionSpec as P

H = 16
C = 256
N = 1024
HD = 16
QB = 256
NQ = N // QB
AQ = 512
NA = N // AQ
KC = 512
NK = N // KC
GROUP = 8
ORDER_HELP = ("order_0", "order_1", "order_2", "help")
EPS = 1e-05
NEG = -1e30
SCALE = HD**-0.5
QSCALE = SCALE * math.log2(math.e)
POINT_SCALE = 2.0 * N**-0.5
F32 = jnp.float32
BF16 = jnp.bfloat16
MESH = pl.DeviceIdType.MESH
VMEM = pltpu.VMEM


def iota(shape, dim):
    return lax.broadcasted_iota(jnp.int32, shape, dim)


def mm(a, b):
    return jnp.dot(a, b, preferred_element_type=F32)


def mm_nt(a, b):
    return lax.dot_general(a, b, (((1,), (1,)), ((), ())), preferred_element_type=F32)


def split3(x):
    hi = x.astype(BF16)
    rest = x - hi.astype(F32)
    mid = rest.astype(BF16)
    lo = (rest - mid.astype(F32)).astype(BF16)
    return hi, mid, lo


def local_kernel(
    raw_ref,
    serial_ref,
    counts_ref,
    gain_ref,
    wqkv_ref,
    wproj_ref,
    og_ref,
    cluster_ref,
    joined_ref,
    pooled_ref,
    gfeats_ref,
    send_ref,
    gsum_ref,
    edge_ref,
    gath_ref,
    hid_ref,
    normed_ref,
    inv_ref,
    pT_ref,
    doT_ref,
    ka_ref,
    va_ref,
    qa_ref,
    vt_ref,
    e_ref,
    ds_ref,
    attT_ref,
    gpT_ref,
    dk_ref,
    dv_ref,
    grad_ref,
    dx_ref,
    bo_ref,
    bo2_ref,
    ids_ref,
    cols_ref,
    kv_ref,
    et_ref,
    dst_ref,
):
    n_live = counts_ref[0, 0]
    gain = gain_ref[...]
    serial_row = serial_ref[...]
    cols_ref[...] = jnp.transpose(jnp.broadcast_to(serial_row.astype(F32), (128, N)))
    lane128 = iota((QB, 128), 1).astype(F32)

    for t in range(4):
        rows = pl.ds(t * QB, QB)
        sc = cols_ref[rows, :]
        onehot = jnp.concatenate(
            [jnp.where(sc == lane128 + float(128 * b), 1.0, 0.0).astype(BF16) for b in range(8)],
            axis=1,
        )
        x = mm(onehot, raw_ref[...])
        gath_ref[rows, :] = x.astype(BF16)
        centred = x - jnp.mean(x, axis=1, keepdims=True)
        inv = lax.rsqrt(jnp.mean(centred * centred, axis=1, keepdims=True) + EPS)
        normed = centred * inv
        normed_ref[rows, :] = normed
        inv_ref[rows, :] = inv
        hid = (normed * gain).astype(BF16)
        hid_ref[rows, :] = hid
        packed = mm(hid, wqkv_ref[...]).astype(BF16)
        pT_ref[:, rows] = jnp.transpose(packed)
        bp = mm_nt(og_ref[rows, :], wproj_ref[...]).astype(BF16)
        bpT = jnp.transpose(bp)
        lane = iota((C, QB), 1) + t * QB
        doT_ref[:, rows] = jnp.where(lane < n_live, bpT.astype(F32), 0.0).astype(BF16)
        kv_ref[rows, :] = packed[:, C:]

    chan = iota((C, C), 0)
    place = iota((C, C), 1)
    spot = place % 64
    for b in range(4):
        cols = pl.ds(b * C, C)
        same = ((place // 64 + 4 * b) == chan // HD) & (spot % HD == chan % HD)
        rep_k = jnp.where(same & (spot < 3 * HD), 1.0, 0.0).astype(BF16)
        rep_v = jnp.where(same & (spot < 2 * HD), 1.0, 0.0).astype(BF16)
        spot_r = iota((1, C), 1) % 64
        ones_k = jnp.where((spot_r >= 48) & (spot_r < 51), 1.0, 0.0)
        ones_v = jnp.where((spot_r >= 32) & (spot_r < 35), 1.0, 0.0)
        dead_k = jnp.where(spot_r == 51, NEG, 0.0)
        for t in range(4):
            rows = pl.ds(t * QB, QB)
            dead = jnp.where((iota((QB, 1), 0) + t * QB) < n_live, 0.0, 1.0)
            ka = mm(kv_ref[rows, :C], rep_k) + ones_k + dead * dead_k
            ka_ref[rows, cols] = ka.astype(BF16)
            va = mm(kv_ref[rows, C:], rep_v) + ones_v
            va_ref[rows, cols] = va.astype(BF16)

    def prep(h, carry):
        q = pT_ref[pl.ds(h * HD, HD), :].astype(F32)
        k = pT_ref[pl.ds(C + h * HD, HD), :].astype(F32)
        v = pT_ref[pl.ds(2 * C + h * HD, HD), :]
        do = doT_ref[pl.ds(h * HD, HD), :]
        q = q * QSCALE
        hi, mid, lo = split3(q)
        row = iota((HD, N), 0)
        tail = jnp.where(row == 3, 1.0, 0.0).astype(BF16)
        zeros = jnp.zeros((64, N), BF16)
        base = pl.multiple_of(h * 128, 128)
        half = pl.multiple_of((h % 2) * 64, 64)
        qa_ref[pl.ds(pl.multiple_of(base + half, 64), 64), :] = jnp.concatenate(
            [hi, mid, lo, tail], axis=0
        )
        qa_ref[pl.ds(pl.multiple_of(base + 64 - half, 64), 64), :] = zeros
        ones = jnp.where(row == 0, 1.0, 0.0).astype(BF16)
        vt_ref[pl.ds(h * 32, 32), :] = jnp.concatenate([v, ones], axis=0)
        q2 = jnp.max(jnp.sum(q * q, axis=0, keepdims=True))
        k2 = jnp.max(jnp.sum(k * k, axis=0, keepdims=True))
        vmax = jnp.max(jnp.abs(v.astype(F32)))
        dmax = jnp.max(jnp.abs(do.astype(F32)))
        tame = (q2 * k2 <= 8100.0) & (vmax <= 4096.0) & (dmax <= 4096.0)

        @pl.when(jnp.logical_not(tame))
        def _():
            lanes = pl.ds(pl.multiple_of((h // 2) * 128, 128), 128)
            for t in range(NQ):
                cols = pl.ds(t * QB, QB)
                peak = jnp.full((1, QB), -jnp.inf, F32)
                for r in range(4):
                    s = mm(ka_ref[pl.ds(r * QB, QB), lanes], qa_ref[pl.ds(base, 128), cols])
                    peak = jnp.maximum(peak, jnp.max(s, axis=0, keepdims=True))
                p_hi, p_mid, p_lo = split3(-peak)
                rowq = iota((HD, QB), 0)
                shift = jnp.where(rowq == 0, p_hi.astype(F32), 0.0)
                shift = jnp.where(rowq == 1, p_mid.astype(F32), shift)
                shift = jnp.where(rowq == 2, p_lo.astype(F32), shift)
                shift = jnp.where(rowq == 3, 1.0, shift)
                at = pl.multiple_of(base + half + 48, 16)
                qa_ref[pl.ds(at, HD), cols] = shift.astype(BF16)

        return carry

    lax.fori_loop(0, H, prep, 0)

    def names(p, j):
        side, t, slot = j // NA, j % NA, j % 2
        h = 2 * p + side
        hrows = pl.ds(pl.multiple_of(h * HD, HD), HD)
        krows = pl.ds(pl.multiple_of(C + h * HD, HD), HD)
        vrows = pl.ds(pl.multiple_of(2 * C + h * HD, HD), HD)
        lanes = pl.ds(pl.multiple_of(p * 128, 128), 128)
        return side, t, slot, h, slice(t * AQ, (t + 1) * AQ), lanes, hrows, krows, vrows

    def keys(r):
        return slice(r * KC, (r + 1) * KC)

    def first_stage(p, j, r):
        side, t, slot, h, cols, lanes, hrows, krows, vrows = names(p, j)
        rhs = qa_ref[pl.ds(pl.multiple_of(h * 128, 128), 128), cols]
        e = jnp.exp2(mm(ka_ref[keys(r), lanes], rhs)).astype(BF16)
        e_ref[slot, keys(r), :] = e
        et_ref[slot, :, keys(r)] = jnp.transpose(e)

    def block(p, j, following):
        side, t, slot, h, cols, lanes, hrows, krows, vrows = names(p, j)
        o_un = mm(vt_ref[pl.ds(pl.multiple_of(h * 32, 32), 32), :], e_ref[slot])
        first_stage(*following, 0)
        l_inv = 1.0 / o_un[HD : HD + 1, :]
        o = o_un[:HD, :] * l_inv
        live = (iota((HD, AQ), 1) + t * AQ) < n_live
        attT_ref[hrows, cols] = jnp.where(live, o, 0.0).astype(BF16)
        do = doT_ref[hrows, cols].astype(F32)
        dl = do * l_inv
        d_hi = dl.astype(BF16)
        d_lo = (dl - d_hi.astype(F32)).astype(BF16)
        cross = -jnp.sum(dl * o, axis=0, keepdims=True)
        c_hi, c_mid, c_lo = split3(cross)
        row = iota((32, AQ), 0)
        tail = jnp.where(row == 0, c_hi.astype(F32), 0.0)
        tail = jnp.where(row == 1, c_mid.astype(F32), tail)
        tail = jnp.where(row == 2, c_lo.astype(F32), tail)
        both = jnp.concatenate([d_hi, d_lo], axis=0)
        zeros = jnp.zeros((64, AQ), BF16)
        parts = [both, tail.astype(BF16)]
        parts = parts + [zeros] if side == 0 else [zeros] + parts
        rhs = jnp.concatenate(parts, axis=0)

        def value_grad(r):
            dv = mm(both, et_ref[slot, :, keys(r)])
            dv = dv[:HD] + dv[HD:]
            if t > 0:
                dv = dv_ref[:, keys(r)] + dv
            if t < NA - 1:
                dv_ref[:, keys(r)] = dv
            else:
                gpT_ref[vrows, keys(r)] = dv.astype(BF16)

        def cotangent(r):
            dp = mm(va_ref[keys(r), lanes], rhs)
            ds = (e_ref[slot, keys(r), :].astype(F32) * dp).astype(BF16)
            ds_ref[slot, keys(r), :] = ds
            dst_ref[slot, :, keys(r)] = jnp.transpose(ds)

        def score_grads(r):
            dk = mm(pT_ref[hrows, cols], dst_ref[slot, :, keys(r)])
            if t > 0:
                dk = dk_ref[:, keys(r)] + dk
            if t < NA - 1:
                dk_ref[:, keys(r)] = dk
            else:
                gpT_ref[krows, keys(r)] = (dk * SCALE).astype(BF16)
            return mm(pT_ref[krows, keys(r)], ds_ref[slot, keys(r), :])

        for r in range(1, NK):
            first_stage(*following, r)
            value_grad(r - 1)
        cotangent(0)
        value_grad(NK - 1)
        dq = jnp.zeros((HD, AQ), F32)
        for r in range(1, NK):
            cotangent(r)
            dq = dq + score_grads(r - 1)
        dq = dq + score_grads(NK - 1)
        gpT_ref[hrows, cols] = (dq * SCALE).astype(BF16)

    for r in range(NK):
        first_stage(0, 0, r)

    def pair(p, carry):
        for j in range(2 * NA):
            if j < 2 * NA - 1:
                block(p, j, (p, j + 1))
            else:
                block(p, j, (jnp.minimum(p + 1, H // 2 - 1), 0))
        return carry

    lax.fori_loop(0, H // 2, pair, 0)

    grad_ref[: 3 * C, :] = mm(gpT_ref[...], hid_ref[...]) * POINT_SCALE
    grad_ref[3 * C :, :] = mm(attT_ref[...], og_ref[...]) * POINT_SCALE
    for half in range(2):
        part = grad_ref[:, half * 128 : (half + 1) * 128].reshape(128, 8, 128)
        send_ref[:, half * 8 : (half + 1) * 8, :] = part.astype(BF16)

    gain_sum = jnp.zeros((1, C), F32)
    for t in range(4):
        rows = pl.ds(t * QB, QB)
        att = jnp.transpose(attT_ref[:, rows])
        bo = gath_ref[rows, :].astype(F32) + mm(att, wproj_ref[...])
        bo_ref[pl.ds(t * QB + 8, QB), :] = bo.astype(BF16).astype(F32)
        gp = jnp.transpose(gpT_ref[:, rows])
        gh = mm_nt(gp, wqkv_ref[...])
        normed = normed_ref[rows, :]
        gain_sum = gain_sum + jnp.sum(gh * normed, axis=0, keepdims=True)
        g = gh * gain
        mean_g = jnp.mean(g, axis=1, keepdims=True)
        mean_c = jnp.mean(g * normed, axis=1, keepdims=True)
        dx = og_ref[rows, :].astype(F32) + inv_ref[rows, :] * (g - mean_g - normed * mean_c)
        dx_ref[rows, :] = dx.astype(BF16)
    gain_sum = gain_sum * POINT_SCALE
    gsum_ref[0] = gain_sum[:, :128]
    gsum_ref[1] = gain_sum[:, 128:]
    for t in range(4):
        spot = iota((QB, N), 0) + t * QB
        onehot = jnp.where(spot == serial_row, 1.0, 0.0).astype(BF16)
        gfeats_ref[pl.ds(t * QB, QB), :] = mm(onehot, dx_ref[...]).astype(BF16)

    ids_ref[8 : N + 8, :] = jnp.transpose(
        jnp.broadcast_to(cluster_ref[...].astype(F32), (128, N))
    )
    ids_ref[:8, :] = jnp.full((8, 128), -1.0, F32)
    ids_ref[N + 8 :, :] = jnp.full((8, 128), -2.0, F32)
    bo_ref[:8, :] = jnp.full((8, C), -jnp.inf, F32)
    bo_ref[N + 8 :, :] = jnp.full((8, C), -jnp.inf, F32)
    span = 128
    wide = span + 16

    def pool(i, carry):
        at = pl.multiple_of(i * span, span)
        ids = ids_ref[pl.ds(at, wide), :]
        shifts = (1, 2, 4, wide - 1, wide - 2, wide - 4)
        same = [pltpu.roll(ids, step, 0) == ids for step in shifts]
        for half in range(2):
            cols = slice(half * 128, (half + 1) * 128)
            m = bo_ref[pl.ds(at, wide), cols]
            for step, ok in zip(shifts, same):
                m = jnp.maximum(m, jnp.where(ok, pltpu.roll(m, step, 0), -jnp.inf))
            bo2_ref[pl.ds(at, span), cols] = m[8 : span + 8]
        return carry

    lax.fori_loop(0, N // span, pool, 0)
    pooled_ref[...] = bo2_ref[...].astype(BF16)
    edge_ref[0, :8, :] = bo2_ref[:8, :]
    edge_ref[1, :8, :] = bo2_ref[N - 8 :, :]
    flag = jnp.full((8, C), joined_ref[0], jnp.int32).astype(F32)
    edge_ref[0, 8:, :] = flag
    edge_ref[1, 8:, :] = flag


def local_part(raw, serial, counts, gain, w_qkv, w_proj, out_grad, cluster, joined):
    shapes = (
        jax.ShapeDtypeStruct((N, C), BF16),
        jax.ShapeDtypeStruct((N, C), BF16),
        jax.ShapeDtypeStruct((128, 16, 128), BF16),
        jax.ShapeDtypeStruct((2, 1, 128), F32),
        jax.ShapeDtypeStruct((2, 16, C), F32),
    )
    vm = pl.BlockSpec(memory_space=VMEM)
    sm = pl.BlockSpec(memory_space=pltpu.SMEM)
    return pl.pallas_call(
        local_kernel,
        out_shape=shapes,
        in_specs=[vm, vm, sm, vm, vm, vm, vm, vm, sm],
        out_specs=[vm] * 5,
        scratch_shapes=[
            VMEM((N, C), BF16),
            VMEM((N, C), BF16),
            VMEM((N, C), F32),
            VMEM((N, 1), F32),
            VMEM((3 * C, N), BF16),
            VMEM((C, N), BF16),
            VMEM((N, 4 * C), BF16),
            VMEM((N, 4 * C), BF16),
            VMEM((H * 128, N), BF16),
            VMEM((H * 32, N), BF16),
            VMEM((2, N, AQ), BF16),
            VMEM((2, N, AQ), BF16),
            VMEM((C, N), BF16),
            VMEM((3 * C, N), BF16),
            VMEM((HD, N), F32),
            VMEM((HD, N), F32),
            VMEM((N, C), F32),
            VMEM((N, C), BF16),
            VMEM((N + 16, C), F32),
            VMEM((N, C), F32),
            VMEM((N + 16, 128), F32),
            VMEM((N, 128), F32),
            VMEM((N, 2 * C), BF16),
            VMEM((2, AQ, N), BF16),
            VMEM((2, AQ, N), BF16),
        ],
        compiler_params=pltpu.CompilerParams(vmem_limit_bytes=46 * 1024 * 1024),
        name="local_part",
    )(raw, serial, counts, gain, w_qkv, w_proj, out_grad, cluster, joined)


def comm_kernel(
    send_ref,
    gsum_ref,
    edge_ref,
    ends_in_ref,
    cluster_ref,
    ends_ref,
    gqkv_ref,
    gproj_ref,
    ggain_ref,
    pair_buf,
    pair_gain,
    edge_buf,
    chip_buf,
    chip_gain,
    rs_buf,
    gain_buf,
    ag_buf,
    out_buf,
    gain_out,
    grad_buf,
    sems,
):
    y = lax.axis_index("order_0")
    x = lax.axis_index("order_1")
    core = lax.axis_index("order_2")
    z = lax.axis_index("help")
    chip = (y * 4 + x) * 4 + z
    shard = ((y * 4 + x) * 2 + core) * 4 + z

    def of_shard(s):
        return (s // 32, (s // 8) % 4, (s // 4) % 2, s % 4)

    def of_chip(r):
        return ((y + r // 16) % 4, (x + (r // 4) % 4) % 4, core, (z + r % 4) % 4)

    partner = (y, x, 1 - core, z)
    following = of_shard((shard + 1) % 128)
    previous = of_shard((shard + 127) % 128)

    barrier = pltpu.get_barrier_semaphore()

    def greet(r, carry):
        pl.semaphore_signal(barrier, inc=1, device_id=of_chip(r), device_id_type=MESH)
        return carry

    lax.fori_loop(1, 64, greet, 0)
    for other in (partner, following, previous):
        pl.semaphore_signal(barrier, inc=1, device_id=other, device_id_type=MESH)
    pl.semaphore_wait(barrier, 66)

    def remote(src, dst, i, device):
        return pltpu.make_async_remote_copy(
            src_ref=src,
            dst_ref=dst,
            send_sem=sems.at[2 * i],
            recv_sem=sems.at[2 * i + 1],
            device_id=device,
            device_id_type=MESH,
        )

    far = 64 * (1 - core)
    pair_copy = remote(send_ref.at[pl.ds(far, 64)], pair_buf, 0, partner)
    pair_copy.start()
    pair_gain_copy = remote(gsum_ref.at[1 - core], pair_gain, 1, partner)
    pair_gain_copy.start()
    ahead = remote(edge_ref.at[1], edge_buf.at[0], 2, following)
    ahead.start()
    back = remote(edge_ref.at[0], edge_buf.at[1], 3, previous)
    back.start()

    pair_copy.wait()
    mine = send_ref[pl.ds(64 * core, 64)].astype(F32) + pair_buf[...].astype(F32)
    chip_buf[...] = mine.astype(BF16)
    pair_gain_copy.wait()
    chip_gain[...] = gsum_ref[core] + pair_gain[...]

    def scatter(r, carry):
        to = of_chip(r)
        other = (to[0] * 4 + to[1]) * 4 + to[3]
        remote(chip_buf.at[other], rs_buf.at[chip], 4, to).start()
        remote(chip_gain, gain_buf.at[chip], 5, to).start()
        return carry

    lax.fori_loop(1, 64, scatter, 0)
    rs_buf[pl.ds(chip, 1)] = chip_buf[pl.ds(chip, 1)]
    gain_buf[pl.ds(chip, 1)] = chip_gain[...][None]

    ahead.wait()
    back.wait()
    ids = jnp.transpose(jnp.broadcast_to(cluster_ref[...].astype(F32), (128, N)))
    first = ids[:8]
    last = ids[N - 8 :]
    linked = (edge_ref[0, 8:9, :128] > 0.0) & (shard > 0)
    head_ok = (first == first[:1]) & linked
    next_joined = edge_buf[1, 8:9, :128] > 0.0
    tail_ok = (last == last[7:8]) & next_joined & (shard < 127)
    for half in range(2):
        cols = slice(half * 128, (half + 1) * 128)
        from_prev = edge_buf[0, 7:8, cols]
        from_next = edge_buf[1, 0:1, cols]
        top = edge_ref[0, 0:8, cols]
        top = jnp.where(head_ok, jnp.maximum(top, from_prev), top)
        low = edge_ref[1, 0:8, cols]
        low = jnp.where(tail_ok, jnp.maximum(low, from_next), low)
        above = ends_in_ref[8:16, cols].astype(F32)
        below = ends_in_ref[16:24, cols].astype(F32)
        ends_ref[:16, cols] = jnp.concatenate([top, above], axis=0).astype(BF16)
        ends_ref[16:, cols] = jnp.concatenate([below, low], axis=0).astype(BF16)

    everything = pl.ds(0, 63)
    for i, (src, dst) in ((4, (ag_buf, rs_buf)), (5, (gain_out, gain_buf))):
        whole = remote(dst.at[everything], dst.at[everything], i, partner)
        whole.wait_recv()
        whole.wait_send()
    total = jnp.sum(rs_buf[...].astype(F32), axis=0)
    ag_buf[pl.ds(chip, 1)] = total.astype(BF16)[None]

    def gather(r, carry):
        remote(ag_buf.at[chip], ag_buf.at[chip], 6, of_chip(r)).start()
        return carry

    lax.fori_loop(1, 64, gather, 0)
    gain_out[pl.ds(core, 1)] = jnp.sum(gain_buf[...], axis=0)[None]
    last_gain = remote(gain_out.at[core], gain_out.at[core], 7, partner)
    last_gain.start()
    whole = remote(ag_buf.at[everything], ag_buf.at[everything], 6, partner)
    whole.wait_recv()
    whole.wait_send()
    last_copy = remote(ag_buf, out_buf.at[core], 8, partner)
    last_copy.start()
    out_buf[pl.ds(core, 1)] = ag_buf[...][None]
    last_gain.wait()
    ggain_ref[:, :128] = gain_out[0]
    ggain_ref[:, 128:] = gain_out[1]
    last_copy.wait()
    for c in range(2):
        for half in range(2):
            part = out_buf[c, :, half * 8 : (half + 1) * 8, :].astype(F32).reshape(512, 128)
            grad_buf[c * 512 : (c + 1) * 512, half * 128 : (half + 1) * 128] = part
    gqkv_ref[...] = jnp.transpose(grad_buf[: 3 * C, :])
    gproj_ref[...] = grad_buf[3 * C :, :]


def comm_part(send, gsum, edge, ends, cluster):
    shapes = (
        jax.ShapeDtypeStruct((32, C), BF16),
        jax.ShapeDtypeStruct((C, 3 * C), F32),
        jax.ShapeDtypeStruct((C, C), F32),
        jax.ShapeDtypeStruct((1, C), F32),
    )
    vm = pl.BlockSpec(memory_space=VMEM)
    return pl.pallas_call(
        comm_kernel,
        out_shape=shapes,
        in_specs=[vm] * 5,
        out_specs=[vm] * 4,
        scratch_shapes=[
            VMEM((64, 16, 128), BF16),
            VMEM((1, 128), F32),
            VMEM((2, 16, C), F32),
            VMEM((64, 16, 128), BF16),
            VMEM((1, 128), F32),
            VMEM((64, 16, 128), BF16),
            VMEM((64, 1, 128), F32),
            VMEM((64, 16, 128), BF16),
            VMEM((2, 64, 16, 128), BF16),
            VMEM((2, 1, 128), F32),
            VMEM((N, C), F32),
            pltpu.SemaphoreType.DMA((18,)),
        ],
        compiler_params=pltpu.CompilerParams(
            collective_id=0, has_side_effects=True, vmem_limit_bytes=16 * 1024 * 1024
        ),
        name="comm_part",
    )(send, gsum, edge, ends, cluster)


def body(raw_feats, serial, counts, norm_gain, w_qkv, w_proj, out_grad, cluster, joined):
    pooled, grad_feats, send, gsum, edge = local_part(
        raw_feats[0], serial, counts, norm_gain[None], w_qkv, w_proj, out_grad[0], cluster, joined
    )
    ends = jnp.concatenate([pooled[:16], pooled[N - 16 :]], axis=0)
    ends, grad_qkv, grad_proj, grad_gain = comm_part(send, gsum, edge, ends, cluster)
    pooled = pooled.at[:16].set(ends[:16]).at[N - 16 :].set(ends[16:])
    return (pooled[None], grad_feats[None], grad_qkv, grad_proj, grad_gain[0])


def solution(mesh):
    torus = Mesh(
        mesh.devices.reshape(4, 4, 2, mesh.shape["help"]), ("order_0", "order_1", "order_2", "help")
    )
    placed = (
        P(ORDER_HELP, None, None),
        P(ORDER_HELP, None),
        P(ORDER_HELP, None),
        P(),
        P(),
        P(),
        P(ORDER_HELP, None, None),
        P(ORDER_HELP, None),
        P(ORDER_HELP),
    )
    return jax.shard_map(
        body,
        mesh=torus,
        in_specs=placed,
        out_specs=(P(ORDER_HELP, None, None), P(ORDER_HELP, None, None), P(), P(), P()),
        check_vma=False,
    )
```

```python
import math

import jax
import jax.numpy as jnp
from jax import lax
from jax.experimental import pallas as pl
from jax.experimental.pallas import tpu as pltpu
from jax.sharding import Mesh
from jax.sharding import PartitionSpec as P

H = 16
C = 256
N = 1024
HD = 16
QB = 256
NQ = N // QB
AQ = 512
NA = N // AQ
KC = 512
NK = N // KC
GROUP = 8
ORDER_HELP = ("order_0", "order_1", "order_2", "help")
EPS = 1e-05
NEG = -1e30
SCALE = HD**-0.5
QSCALE = SCALE * math.log2(math.e)
POINT_SCALE = 2.0 * N**-0.5
F32 = jnp.float32
BF16 = jnp.bfloat16
MESH = pl.DeviceIdType.MESH
VMEM = pltpu.VMEM


def iota(shape, dim):
    return lax.broadcasted_iota(jnp.int32, shape, dim)


def mm(a, b):
    return jnp.dot(a, b, preferred_element_type=F32)


def mm_nt(a, b):
    return lax.dot_general(a, b, (((1,), (1,)), ((), ())), preferred_element_type=F32)


def split3(x):
    hi = x.astype(BF16)
    rest = x - hi.astype(F32)
    mid = rest.astype(BF16)
    lo = (rest - mid.astype(F32)).astype(BF16)
    return hi, mid, lo


def local_kernel(
    raw_ref,
    serial_ref,
    counts_ref,
    gain_ref,
    wqkv_ref,
    wproj_ref,
    og_ref,
    cluster_ref,
    joined_ref,
    pooled_ref,
    gfeats_ref,
    send_ref,
    gsum_ref,
    edge_ref,
    rim_ref,
    gath_ref,
    hid_ref,
    normed_ref,
    inv_ref,
    pT_ref,
    doT_ref,
    ka_ref,
    va_ref,
    qa_ref,
    vt_ref,
    e_ref,
    ds_ref,
    attT_ref,
    gpT_ref,
    dk_ref,
    dv_ref,
    grad_ref,
    dx_ref,
    bo_ref,
    bo2_ref,
    ids_ref,
    cols_ref,
    kv_ref,
    et_ref,
    dst_ref,
):
    n_live = counts_ref[0, 0]
    gain = gain_ref[...]
    serial_row = serial_ref[...]
    cols_ref[...] = jnp.transpose(jnp.broadcast_to(serial_row.astype(F32), (128, N)))
    lane128 = iota((QB, 128), 1).astype(F32)

    for t in range(4):
        rows = pl.ds(t * QB, QB)
        sc = cols_ref[rows, :]
        onehot = jnp.concatenate(
            [jnp.where(sc == lane128 + float(128 * b), 1.0, 0.0).astype(BF16) for b in range(8)],
            axis=1,
        )
        x = mm(onehot, raw_ref[...])
        gath_ref[rows, :] = x.astype(BF16)
        centred = x - jnp.mean(x, axis=1, keepdims=True)
        inv = lax.rsqrt(jnp.mean(centred * centred, axis=1, keepdims=True) + EPS)
        normed = centred * inv
        normed_ref[rows, :] = normed
        inv_ref[rows, :] = inv
        hid = (normed * gain).astype(BF16)
        hid_ref[rows, :] = hid
        packed = mm(hid, wqkv_ref[...]).astype(BF16)
        pT_ref[:, rows] = jnp.transpose(packed)
        bp = mm_nt(og_ref[rows, :], wproj_ref[...]).astype(BF16)
        bpT = jnp.transpose(bp)
        lane = iota((C, QB), 1) + t * QB
        doT_ref[:, rows] = jnp.where(lane < n_live, bpT.astype(F32), 0.0).astype(BF16)
        kv_ref[rows, :] = packed[:, C:]

    chan = iota((C, C), 0)
    place = iota((C, C), 1)
    spot = place % 64
    for b in range(4):
        cols = pl.ds(b * C, C)
        same = ((place // 64 + 4 * b) == chan // HD) & (spot % HD == chan % HD)
        rep_k = jnp.where(same & (spot < 3 * HD), 1.0, 0.0).astype(BF16)
        rep_v = jnp.where(same & (spot < 2 * HD), 1.0, 0.0).astype(BF16)
        spot_r = iota((1, C), 1) % 64
        ones_k = jnp.where((spot_r >= 48) & (spot_r < 51), 1.0, 0.0)
        ones_v = jnp.where((spot_r >= 32) & (spot_r < 35), 1.0, 0.0)
        dead_k = jnp.where(spot_r == 51, NEG, 0.0)
        for t in range(4):
            rows = pl.ds(t * QB, QB)
            dead = jnp.where((iota((QB, 1), 0) + t * QB) < n_live, 0.0, 1.0)
            ka = mm(kv_ref[rows, :C], rep_k) + ones_k + dead * dead_k
            ka_ref[rows, cols] = ka.astype(BF16)
            va = mm(kv_ref[rows, C:], rep_v) + ones_v
            va_ref[rows, cols] = va.astype(BF16)

    def prep(h, carry):
        q = pT_ref[pl.ds(h * HD, HD), :].astype(F32)
        k = pT_ref[pl.ds(C + h * HD, HD), :].astype(F32)
        v = pT_ref[pl.ds(2 * C + h * HD, HD), :]
        do = doT_ref[pl.ds(h * HD, HD), :]
        q = q * QSCALE
        hi, mid, lo = split3(q)
        row = iota((HD, N), 0)
        tail = jnp.where(row == 3, 1.0, 0.0).astype(BF16)
        zeros = jnp.zeros((64, N), BF16)
        base = pl.multiple_of(h * 128, 128)
        half = pl.multiple_of((h % 2) * 64, 64)
        qa_ref[pl.ds(pl.multiple_of(base + half, 64), 64), :] = jnp.concatenate(
            [hi, mid, lo, tail], axis=0
        )
        qa_ref[pl.ds(pl.multiple_of(base + 64 - half, 64), 64), :] = zeros
        ones = jnp.where(row == 0, 1.0, 0.0).astype(BF16)
        vt_ref[pl.ds(h * 32, 32), :] = jnp.concatenate([v, ones], axis=0)
        q2 = jnp.max(jnp.sum(q * q, axis=0, keepdims=True))
        k2 = jnp.max(jnp.sum(k * k, axis=0, keepdims=True))
        vmax = jnp.max(jnp.abs(v.astype(F32)))
        dmax = jnp.max(jnp.abs(do.astype(F32)))
        tame = (q2 * k2 <= 8100.0) & (vmax <= 4096.0) & (dmax <= 4096.0)

        @pl.when(jnp.logical_not(tame))
        def _():
            lanes = pl.ds(pl.multiple_of((h // 2) * 128, 128), 128)
            for t in range(NQ):
                cols = pl.ds(t * QB, QB)
                peak = jnp.full((1, QB), -jnp.inf, F32)
                for r in range(4):
                    s = mm(ka_ref[pl.ds(r * QB, QB), lanes], qa_ref[pl.ds(base, 128), cols])
                    peak = jnp.maximum(peak, jnp.max(s, axis=0, keepdims=True))
                p_hi, p_mid, p_lo = split3(-peak)
                rowq = iota((HD, QB), 0)
                shift = jnp.where(rowq == 0, p_hi.astype(F32), 0.0)
                shift = jnp.where(rowq == 1, p_mid.astype(F32), shift)
                shift = jnp.where(rowq == 2, p_lo.astype(F32), shift)
                shift = jnp.where(rowq == 3, 1.0, shift)
                at = pl.multiple_of(base + half + 48, 16)
                qa_ref[pl.ds(at, HD), cols] = shift.astype(BF16)

        return carry

    lax.fori_loop(0, H, prep, 0)

    def names(p, j):
        side, t, slot = j // NA, j % NA, j % 2
        h = 2 * p + side
        hrows = pl.ds(pl.multiple_of(h * HD, HD), HD)
        krows = pl.ds(pl.multiple_of(C + h * HD, HD), HD)
        vrows = pl.ds(pl.multiple_of(2 * C + h * HD, HD), HD)
        lanes = pl.ds(pl.multiple_of(p * 128, 128), 128)
        return side, t, slot, h, slice(t * AQ, (t + 1) * AQ), lanes, hrows, krows, vrows

    def keys(r):
        return slice(r * KC, (r + 1) * KC)

    def first_stage(p, j, r):
        side, t, slot, h, cols, lanes, hrows, krows, vrows = names(p, j)
        rhs = qa_ref[pl.ds(pl.multiple_of(h * 128, 128), 128), cols]
        e = jnp.exp2(mm(ka_ref[keys(r), lanes], rhs)).astype(BF16)
        e_ref[slot, keys(r), :] = e
        et_ref[slot, :, keys(r)] = jnp.transpose(e)

    def block(p, j, following):
        side, t, slot, h, cols, lanes, hrows, krows, vrows = names(p, j)
        o_un = mm(vt_ref[pl.ds(pl.multiple_of(h * 32, 32), 32), :], e_ref[slot])
        first_stage(*following, 0)
        l_inv = 1.0 / o_un[HD : HD + 1, :]
        o = o_un[:HD, :] * l_inv
        live = (iota((HD, AQ), 1) + t * AQ) < n_live
        attT_ref[hrows, cols] = jnp.where(live, o, 0.0).astype(BF16)
        do = doT_ref[hrows, cols].astype(F32)
        dl = do * l_inv
        d_hi = dl.astype(BF16)
        d_lo = (dl - d_hi.astype(F32)).astype(BF16)
        cross = -jnp.sum(dl * o, axis=0, keepdims=True)
        c_hi, c_mid, c_lo = split3(cross)
        row = iota((32, AQ), 0)
        tail = jnp.where(row == 0, c_hi.astype(F32), 0.0)
        tail = jnp.where(row == 1, c_mid.astype(F32), tail)
        tail = jnp.where(row == 2, c_lo.astype(F32), tail)
        both = jnp.concatenate([d_hi, d_lo], axis=0)
        zeros = jnp.zeros((64, AQ), BF16)
        parts = [both, tail.astype(BF16)]
        parts = parts + [zeros] if side == 0 else [zeros] + parts
        rhs = jnp.concatenate(parts, axis=0)

        def value_grad(r):
            dv = mm(both, et_ref[slot, :, keys(r)])
            dv = dv[:HD] + dv[HD:]
            if t > 0:
                dv = dv_ref[:, keys(r)] + dv
            if t < NA - 1:
                dv_ref[:, keys(r)] = dv
            else:
                gpT_ref[vrows, keys(r)] = dv.astype(BF16)

        def cotangent(r):
            dp = mm(va_ref[keys(r), lanes], rhs)
            ds = (e_ref[slot, keys(r), :].astype(F32) * dp).astype(BF16)
            ds_ref[slot, keys(r), :] = ds
            dst_ref[slot, :, keys(r)] = jnp.transpose(ds)

        def score_grads(r):
            dk = mm(pT_ref[hrows, cols], dst_ref[slot, :, keys(r)])
            if t > 0:
                dk = dk_ref[:, keys(r)] + dk
            if t < NA - 1:
                dk_ref[:, keys(r)] = dk
            else:
                gpT_ref[krows, keys(r)] = (dk * SCALE).astype(BF16)
            return mm(pT_ref[krows, keys(r)], ds_ref[slot, keys(r), :])

        for r in range(1, NK):
            first_stage(*following, r)
            value_grad(r - 1)
        cotangent(0)
        value_grad(NK - 1)
        dq = jnp.zeros((HD, AQ), F32)
        for r in range(1, NK):
            cotangent(r)
            dq = dq + score_grads(r - 1)
        dq = dq + score_grads(NK - 1)
        gpT_ref[hrows, cols] = (dq * SCALE).astype(BF16)

    for r in range(NK):
        first_stage(0, 0, r)

    def pair(p, carry):
        for j in range(2 * NA):
            if j < 2 * NA - 1:
                block(p, j, (p, j + 1))
            else:
                block(p, j, (jnp.minimum(p + 1, H // 2 - 1), 0))
        return carry

    lax.fori_loop(0, H // 2, pair, 0)

    grad_ref[: 3 * C, :] = mm(gpT_ref[...], hid_ref[...]) * POINT_SCALE
    grad_ref[3 * C :, :] = mm(attT_ref[...], og_ref[...]) * POINT_SCALE
    for half in range(2):
        part = grad_ref[:, half * 128 : (half + 1) * 128].reshape(128, 8, 128)
        send_ref[:, half * 8 : (half + 1) * 8, :] = part.astype(BF16)

    gain_sum = jnp.zeros((1, C), F32)
    for t in range(4):
        rows = pl.ds(t * QB, QB)
        att = jnp.transpose(attT_ref[:, rows])
        bo = gath_ref[rows, :].astype(F32) + mm(att, wproj_ref[...])
        bo_ref[pl.ds(t * QB + 8, QB), :] = bo.astype(BF16).astype(F32)
        gp = jnp.transpose(gpT_ref[:, rows])
        gh = mm_nt(gp, wqkv_ref[...])
        normed = normed_ref[rows, :]
        gain_sum = gain_sum + jnp.sum(gh * normed, axis=0, keepdims=True)
        g = gh * gain
        mean_g = jnp.mean(g, axis=1, keepdims=True)
        mean_c = jnp.mean(g * normed, axis=1, keepdims=True)
        dx = og_ref[rows, :].astype(F32) + inv_ref[rows, :] * (g - mean_g - normed * mean_c)
        dx_ref[rows, :] = dx.astype(BF16)
    gain_sum = gain_sum * POINT_SCALE
    gsum_ref[0] = gain_sum[:, :128]
    gsum_ref[1] = gain_sum[:, 128:]
    for t in range(4):
        spot = iota((QB, N), 0) + t * QB
        onehot = jnp.where(spot == serial_row, 1.0, 0.0).astype(BF16)
        gfeats_ref[pl.ds(t * QB, QB), :] = mm(onehot, dx_ref[...]).astype(BF16)

    ids_ref[8 : N + 8, :] = jnp.transpose(
        jnp.broadcast_to(cluster_ref[...].astype(F32), (128, N))
    )
    ids_ref[:8, :] = jnp.full((8, 128), -1.0, F32)
    ids_ref[N + 8 :, :] = jnp.full((8, 128), -2.0, F32)
    bo_ref[:8, :] = jnp.full((8, C), -jnp.inf, F32)
    bo_ref[N + 8 :, :] = jnp.full((8, C), -jnp.inf, F32)
    span = 128
    wide = span + 16

    def pool(i, carry):
        at = pl.multiple_of(i * span, span)
        ids = ids_ref[pl.ds(at, wide), :]
        shifts = (1, 2, 4, wide - 1, wide - 2, wide - 4)
        same = [pltpu.roll(ids, step, 0) == ids for step in shifts]
        for half in range(2):
            cols = slice(half * 128, (half + 1) * 128)
            m = bo_ref[pl.ds(at, wide), cols]
            for step, ok in zip(shifts, same):
                m = jnp.maximum(m, jnp.where(ok, pltpu.roll(m, step, 0), -jnp.inf))
            bo2_ref[pl.ds(at, span), cols] = m[8 : span + 8]
        return carry

    lax.fori_loop(0, N // span, pool, 0)
    pooled_ref[...] = bo2_ref[...].astype(BF16)
    rim_ref[:16, :] = bo2_ref[:16, :].astype(BF16)
    rim_ref[16:, :] = bo2_ref[N - 16 :, :].astype(BF16)
    edge_ref[0, :8, :] = bo2_ref[:8, :]
    edge_ref[1, :8, :] = bo2_ref[N - 8 :, :]
    flag = jnp.full((8, C), joined_ref[0], jnp.int32).astype(F32)
    edge_ref[0, 8:, :] = flag
    edge_ref[1, 8:, :] = flag


def local_part(raw, serial, counts, gain, w_qkv, w_proj, out_grad, cluster, joined):
    shapes = (
        jax.ShapeDtypeStruct((N, C), BF16),
        jax.ShapeDtypeStruct((N, C), BF16),
        jax.ShapeDtypeStruct((128, 16, 128), BF16),
        jax.ShapeDtypeStruct((2, 1, 128), F32),
        jax.ShapeDtypeStruct((2, 16, C), F32),
        jax.ShapeDtypeStruct((32, C), BF16),
    )
    vm = pl.BlockSpec(memory_space=VMEM)
    sm = pl.BlockSpec(memory_space=pltpu.SMEM)
    return pl.pallas_call(
        local_kernel,
        out_shape=shapes,
        in_specs=[vm, vm, sm, vm, vm, vm, vm, vm, sm],
        out_specs=[vm] * 6,
        scratch_shapes=[
            VMEM((N, C), BF16),
            VMEM((N, C), BF16),
            VMEM((N, C), F32),
            VMEM((N, 1), F32),
            VMEM((3 * C, N), BF16),
            VMEM((C, N), BF16),
            VMEM((N, 4 * C), BF16),
            VMEM((N, 4 * C), BF16),
            VMEM((H * 128, N), BF16),
            VMEM((H * 32, N), BF16),
            VMEM((2, N, AQ), BF16),
            VMEM((2, N, AQ), BF16),
            VMEM((C, N), BF16),
            VMEM((3 * C, N), BF16),
            VMEM((HD, N), F32),
            VMEM((HD, N), F32),
            VMEM((N, C), F32),
            VMEM((N, C), BF16),
            VMEM((N + 16, C), F32),
            VMEM((N, C), F32),
            VMEM((N + 16, 128), F32),
            VMEM((N, 128), F32),
            VMEM((N, 2 * C), BF16),
            VMEM((2, AQ, N), BF16),
            VMEM((2, AQ, N), BF16),
        ],
        compiler_params=pltpu.CompilerParams(vmem_limit_bytes=56 * 1024 * 1024),
        name="local_part",
    )(raw, serial, counts, gain, w_qkv, w_proj, out_grad, cluster, joined)


def comm_kernel(
    send_ref,
    gsum_ref,
    edge_ref,
    ends_in_ref,
    cluster_ref,
    ends_ref,
    gqkv_ref,
    gproj_ref,
    ggain_ref,
    pair_buf,
    pair_gain,
    edge_buf,
    chip_buf,
    chip_gain,
    rs_buf,
    gain_buf,
    ag_buf,
    out_buf,
    gain_out,
    grad_buf,
    sems,
):
    y = lax.axis_index("order_0")
    x = lax.axis_index("order_1")
    core = lax.axis_index("order_2")
    z = lax.axis_index("help")
    chip = (y * 4 + x) * 4 + z
    shard = ((y * 4 + x) * 2 + core) * 4 + z

    def of_shard(s):
        return (s // 32, (s // 8) % 4, (s // 4) % 2, s % 4)

    def of_chip(r):
        return ((y + r // 16) % 4, (x + (r // 4) % 4) % 4, core, (z + r % 4) % 4)

    partner = (y, x, 1 - core, z)
    following = of_shard((shard + 1) % 128)
    previous = of_shard((shard + 127) % 128)

    barrier = pltpu.get_barrier_semaphore()

    def greet(r, carry):
        pl.semaphore_signal(barrier, inc=1, device_id=of_chip(r), device_id_type=MESH)
        return carry

    lax.fori_loop(1, 64, greet, 0)
    for other in (partner, following, previous):
        pl.semaphore_signal(barrier, inc=1, device_id=other, device_id_type=MESH)
    pl.semaphore_wait(barrier, 66)

    def remote(src, dst, i, device):
        return pltpu.make_async_remote_copy(
            src_ref=src,
            dst_ref=dst,
            send_sem=sems.at[2 * i],
            recv_sem=sems.at[2 * i + 1],
            device_id=device,
            device_id_type=MESH,
        )

    far = 64 * (1 - core)
    pair_copy = remote(send_ref.at[pl.ds(far, 64)], pair_buf, 0, partner)
    pair_copy.start()
    pair_gain_copy = remote(gsum_ref.at[1 - core], pair_gain, 1, partner)
    pair_gain_copy.start()
    ahead = remote(edge_ref.at[1], edge_buf.at[0], 2, following)
    ahead.start()
    back = remote(edge_ref.at[0], edge_buf.at[1], 3, previous)
    back.start()

    pair_copy.wait()
    mine = send_ref[pl.ds(64 * core, 64)].astype(F32) + pair_buf[...].astype(F32)
    chip_buf[...] = mine.astype(BF16)
    pair_gain_copy.wait()
    chip_gain[...] = gsum_ref[core] + pair_gain[...]

    def scatter(r, carry):
        to = of_chip(r)
        other = (to[0] * 4 + to[1]) * 4 + to[3]
        remote(chip_buf.at[other], rs_buf.at[chip], 4, to).start()
        remote(chip_gain, gain_buf.at[chip], 5, to).start()
        return carry

    lax.fori_loop(1, 64, scatter, 0)
    rs_buf[pl.ds(chip, 1)] = chip_buf[pl.ds(chip, 1)]
    gain_buf[pl.ds(chip, 1)] = chip_gain[...][None]

    ahead.wait()
    back.wait()
    ids = jnp.transpose(jnp.broadcast_to(cluster_ref[...].astype(F32), (128, N)))
    first = ids[:8]
    last = ids[N - 8 :]
    linked = (edge_ref[0, 8:9, :128] > 0.0) & (shard > 0)
    head_ok = (first == first[:1]) & linked
    next_joined = edge_buf[1, 8:9, :128] > 0.0
    tail_ok = (last == last[7:8]) & next_joined & (shard < 127)
    for half in range(2):
        cols = slice(half * 128, (half + 1) * 128)
        from_prev = edge_buf[0, 7:8, cols]
        from_next = edge_buf[1, 0:1, cols]
        top = edge_ref[0, 0:8, cols]
        top = jnp.where(head_ok, jnp.maximum(top, from_prev), top)
        low = edge_ref[1, 0:8, cols]
        low = jnp.where(tail_ok, jnp.maximum(low, from_next), low)
        above = ends_in_ref[8:16, cols].astype(F32)
        below = ends_in_ref[16:24, cols].astype(F32)
        ends_ref[:16, cols] = jnp.concatenate([top, above], axis=0).astype(BF16)
        ends_ref[16:, cols] = jnp.concatenate([below, low], axis=0).astype(BF16)

    everything = pl.ds(0, 63)
    for i, (src, dst) in ((4, (ag_buf, rs_buf)), (5, (gain_out, gain_buf))):
        whole = remote(dst.at[everything], dst.at[everything], i, partner)
        whole.wait_recv()
        whole.wait_send()
    total = jnp.sum(rs_buf[...].astype(F32), axis=0)
    ag_buf[pl.ds(chip, 1)] = total.astype(BF16)[None]

    def gather(r, carry):
        remote(ag_buf.at[chip], ag_buf.at[chip], 6, of_chip(r)).start()
        return carry

    lax.fori_loop(1, 64, gather, 0)
    gain_out[pl.ds(core, 1)] = jnp.sum(gain_buf[...], axis=0)[None]
    last_gain = remote(gain_out.at[core], gain_out.at[core], 7, partner)
    last_gain.start()
    whole = remote(ag_buf.at[everything], ag_buf.at[everything], 6, partner)
    whole.wait_recv()
    whole.wait_send()
    last_copy = remote(ag_buf, out_buf.at[core], 8, partner)
    last_copy.start()
    out_buf[pl.ds(core, 1)] = ag_buf[...][None]
    last_gain.wait()
    ggain_ref[:, :128] = gain_out[0]
    ggain_ref[:, 128:] = gain_out[1]
    last_copy.wait()
    for c in range(2):
        for half in range(2):
            part = out_buf[c, :, half * 8 : (half + 1) * 8, :].astype(F32).reshape(512, 128)
            grad_buf[c * 512 : (c + 1) * 512, half * 128 : (half + 1) * 128] = part
    gqkv_ref[...] = jnp.transpose(grad_buf[: 3 * C, :])
    gproj_ref[...] = grad_buf[3 * C :, :]


def comm_part(send, gsum, edge, ends, cluster):
    shapes = (
        jax.ShapeDtypeStruct((32, C), BF16),
        jax.ShapeDtypeStruct((C, 3 * C), F32),
        jax.ShapeDtypeStruct((C, C), F32),
        jax.ShapeDtypeStruct((1, C), F32),
    )
    vm = pl.BlockSpec(memory_space=VMEM)
    return pl.pallas_call(
        comm_kernel,
        out_shape=shapes,
        in_specs=[vm] * 5,
        out_specs=[vm] * 4,
        scratch_shapes=[
            VMEM((64, 16, 128), BF16),
            VMEM((1, 128), F32),
            VMEM((2, 16, C), F32),
            VMEM((64, 16, 128), BF16),
            VMEM((1, 128), F32),
            VMEM((64, 16, 128), BF16),
            VMEM((64, 1, 128), F32),
            VMEM((64, 16, 128), BF16),
            VMEM((2, 64, 16, 128), BF16),
            VMEM((2, 1, 128), F32),
            VMEM((N, C), F32),
            pltpu.SemaphoreType.DMA((18,)),
        ],
        compiler_params=pltpu.CompilerParams(
            collective_id=0, has_side_effects=True, vmem_limit_bytes=32 * 1024 * 1024
        ),
        name="comm_part",
    )(send, gsum, edge, ends, cluster)


def body(raw_feats, serial, counts, norm_gain, w_qkv, w_proj, out_grad, cluster, joined):
    pooled, grad_feats, send, gsum, edge, ends = local_part(
        raw_feats[0], serial, counts, norm_gain[None], w_qkv, w_proj, out_grad[0], cluster, joined
    )
    ends, grad_qkv, grad_proj, grad_gain = comm_part(send, gsum, edge, ends, cluster)
    pooled = pooled.at[:16].set(ends[:16]).at[N - 16 :].set(ends[16:])
    return (pooled[None], grad_feats[None], grad_qkv, grad_proj, grad_gain[0])


def solution(mesh):
    torus = Mesh(
        mesh.devices.reshape(4, 4, 2, mesh.shape["help"]), ("order_0", "order_1", "order_2", "help")
    )
    placed = (
        P(ORDER_HELP, None, None),
        P(ORDER_HELP, None),
        P(ORDER_HELP, None),
        P(),
        P(),
        P(),
        P(ORDER_HELP, None, None),
        P(ORDER_HELP, None),
        P(ORDER_HELP),
    )
    return jax.shard_map(
        body,
        mesh=torus,
        in_specs=placed,
        out_specs=(P(ORDER_HELP, None, None), P(ORDER_HELP, None, None), P(), P(), P()),
        check_vma=False,
    )
```

```python
import math

import jax
import jax.numpy as jnp
from jax import lax
from jax.experimental import pallas as pl
from jax.experimental.pallas import tpu as pltpu
from jax.sharding import Mesh
from jax.sharding import PartitionSpec as P

H = 16
C = 256
N = 1024
HD = 16
QB = 256
NQ = N // QB
AQ = 1024
NA = N // AQ
LAG = False
GROUP = 8
ORDER_HELP = ("order_0", "order_1", "order_2", "help")
EPS = 1e-05
NEG = -1e30
SCALE = HD**-0.5
QSCALE = SCALE * math.log2(math.e)
POINT_SCALE = 2.0 * N**-0.5
F32 = jnp.float32
BF16 = jnp.bfloat16
MESH = pl.DeviceIdType.MESH
VMEM = pltpu.VMEM


def iota(shape, dim):
    return lax.broadcasted_iota(jnp.int32, shape, dim)


def mm(a, b):
    return jnp.dot(a, b, preferred_element_type=F32)


def mm_nt(a, b):
    return lax.dot_general(a, b, (((1,), (1,)), ((), ())), preferred_element_type=F32)


def split3(x):
    hi = x.astype(BF16)
    rest = x - hi.astype(F32)
    mid = rest.astype(BF16)
    lo = (rest - mid.astype(F32)).astype(BF16)
    return hi, mid, lo


def local_kernel(
    raw_ref,
    serial_ref,
    counts_ref,
    gain_ref,
    wqkv_ref,
    wproj_ref,
    og_ref,
    cluster_ref,
    joined_ref,
    pooled_ref,
    gfeats_ref,
    send_ref,
    gsum_ref,
    edge_ref,
    gath_ref,
    hid_ref,
    normed_ref,
    inv_ref,
    pT_ref,
    doT_ref,
    ka_ref,
    va_ref,
    qa_ref,
    vt_ref,
    e_ref,
    ds_ref,
    attT_ref,
    gpT_ref,
    dk_ref,
    dv_ref,
    grad_ref,
    dx_ref,
    bo_ref,
    bo2_ref,
    ids_ref,
    cols_ref,
    kv_ref,
    et_ref,
    dst_ref,
):
    n_live = counts_ref[0, 0]
    gain = gain_ref[...]
    serial_row = serial_ref[...]
    cols_ref[...] = jnp.transpose(jnp.broadcast_to(serial_row.astype(F32), (128, N)))
    lane128 = iota((QB, 128), 1).astype(F32)

    for t in range(4):
        rows = pl.ds(t * QB, QB)
        sc = cols_ref[rows, :]
        onehot = jnp.concatenate(
            [jnp.where(sc == lane128 + float(128 * b), 1.0, 0.0).astype(BF16) for b in range(8)],
            axis=1,
        )
        x = mm(onehot, raw_ref[...])
        gath_ref[rows, :] = x.astype(BF16)
        centred = x - jnp.mean(x, axis=1, keepdims=True)
        inv = lax.rsqrt(jnp.mean(centred * centred, axis=1, keepdims=True) + EPS)
        normed = centred * inv
        normed_ref[rows, :] = normed
        inv_ref[rows, :] = inv
        hid = (normed * gain).astype(BF16)
        hid_ref[rows, :] = hid
        packed = mm(hid, wqkv_ref[...]).astype(BF16)
        pT_ref[:, rows] = jnp.transpose(packed)
        bp = mm_nt(og_ref[rows, :], wproj_ref[...]).astype(BF16)
        bpT = jnp.transpose(bp)
        lane = iota((C, QB), 1) + t * QB
        doT_ref[:, rows] = jnp.where(lane < n_live, bpT.astype(F32), 0.0).astype(BF16)
        kv_ref[rows, :] = packed[:, C:]

    chan = iota((C, C), 0)
    place = iota((C, C), 1)
    spot = place % 64
    for b in range(4):
        cols = pl.ds(b * C, C)
        same = ((place // 64 + 4 * b) == chan // HD) & (spot % HD == chan % HD)
        rep_k = jnp.where(same & (spot < 3 * HD), 1.0, 0.0).astype(BF16)
        rep_v = jnp.where(same & (spot < 2 * HD), 1.0, 0.0).astype(BF16)
        spot_r = iota((1, C), 1) % 64
        ones_k = jnp.where((spot_r >= 48) & (spot_r < 51), 1.0, 0.0)
        ones_v = jnp.where((spot_r >= 32) & (spot_r < 35), 1.0, 0.0)
        dead_k = jnp.where(spot_r == 51, NEG, 0.0)
        for t in range(4):
            rows = pl.ds(t * QB, QB)
            dead = jnp.where((iota((QB, 1), 0) + t * QB) < n_live, 0.0, 1.0)
            ka = mm(kv_ref[rows, :C], rep_k) + ones_k + dead * dead_k
            ka_ref[rows, cols] = ka.astype(BF16)
            va = mm(kv_ref[rows, C:], rep_v) + ones_v
            va_ref[rows, cols] = va.astype(BF16)

    def prep(h, carry):
        q = pT_ref[pl.ds(h * HD, HD), :].astype(F32)
        k = pT_ref[pl.ds(C + h * HD, HD), :].astype(F32)
        v = pT_ref[pl.ds(2 * C + h * HD, HD), :]
        do = doT_ref[pl.ds(h * HD, HD), :]
        q = q * QSCALE
        hi, mid, lo = split3(q)
        row = iota((HD, N), 0)
        tail = jnp.where(row == 3, 1.0, 0.0).astype(BF16)
        zeros = jnp.zeros((64, N), BF16)
        base = pl.multiple_of(h * 128, 128)
        half = pl.multiple_of((h % 2) * 64, 64)
        qa_ref[pl.ds(pl.multiple_of(base + half, 64), 64), :] = jnp.concatenate(
            [hi, mid, lo, tail], axis=0
        )
        qa_ref[pl.ds(pl.multiple_of(base + 64 - half, 64), 64), :] = zeros
        ones = jnp.where(row == 0, 1.0, 0.0).astype(BF16)
        vt_ref[pl.ds(h * 32, 32), :] = jnp.concatenate([v, ones], axis=0)
        q2 = jnp.max(jnp.sum(q * q, axis=0, keepdims=True))
        k2 = jnp.max(jnp.sum(k * k, axis=0, keepdims=True))
        vmax = jnp.max(jnp.abs(v.astype(F32)))
        dmax = jnp.max(jnp.abs(do.astype(F32)))
        tame = (q2 * k2 <= 8100.0) & (vmax <= 4096.0) & (dmax <= 4096.0)

        @pl.when(jnp.logical_not(tame))
        def _():
            lanes = pl.ds(pl.multiple_of((h // 2) * 128, 128), 128)
            for t in range(NQ):
                cols = pl.ds(t * QB, QB)
                peak = jnp.full((1, QB), -jnp.inf, F32)
                for r in range(4):
                    s = mm(ka_ref[pl.ds(r * QB, QB), lanes], qa_ref[pl.ds(base, 128), cols])
                    peak = jnp.maximum(peak, jnp.max(s, axis=0, keepdims=True))
                p_hi, p_mid, p_lo = split3(-peak)
                rowq = iota((HD, QB), 0)
                shift = jnp.where(rowq == 0, p_hi.astype(F32), 0.0)
                shift = jnp.where(rowq == 1, p_mid.astype(F32), shift)
                shift = jnp.where(rowq == 2, p_lo.astype(F32), shift)
                shift = jnp.where(rowq == 3, 1.0, shift)
                at = pl.multiple_of(base + half + 48, 16)
                qa_ref[pl.ds(at, HD), cols] = shift.astype(BF16)

        return carry

    lax.fori_loop(0, H, prep, 0)

    def names(p, j):
        side, t, slot = j // NA, j % NA, j % 2
        h = 2 * p + side
        hrows = pl.ds(pl.multiple_of(h * HD, HD), HD)
        krows = pl.ds(pl.multiple_of(C + h * HD, HD), HD)
        vrows = pl.ds(pl.multiple_of(2 * C + h * HD, HD), HD)
        lanes = pl.ds(pl.multiple_of(p * 128, 128), 128)
        return side, t, slot, h, slice(t * AQ, (t + 1) * AQ), lanes, hrows, krows, vrows

    def first_stage(p, j):
        side, t, slot, h, cols, lanes, hrows, krows, vrows = names(p, j)
        rhs = qa_ref[pl.ds(pl.multiple_of(h * 128, 128), 128), cols]
        s = mm(ka_ref[:, lanes], rhs)
        e = jnp.exp2(s).astype(BF16)
        e_ref[slot] = e
        et_ref[slot] = jnp.transpose(e)

    def outputs(p, j):
        side, t, slot, h, cols, lanes, hrows, krows, vrows = names(p, j)
        return mm(vt_ref[pl.ds(pl.multiple_of(h * 32, 32), 32), :], e_ref[slot])

    def cotangents(p, j, o_un):
        side, t, slot, h, cols, lanes, hrows, krows, vrows = names(p, j)
        l_inv = 1.0 / o_un[HD : HD + 1, :]
        o = o_un[:HD, :] * l_inv
        live = (iota((HD, AQ), 1) + t * AQ) < n_live
        attT_ref[hrows, cols] = jnp.where(live, o, 0.0).astype(BF16)
        do = doT_ref[hrows, cols].astype(F32)
        dl = do * l_inv
        d_hi = dl.astype(BF16)
        d_lo = (dl - d_hi.astype(F32)).astype(BF16)
        cross = -jnp.sum(dl * o, axis=0, keepdims=True)
        c_hi, c_mid, c_lo = split3(cross)
        row = iota((32, AQ), 0)
        tail = jnp.where(row == 0, c_hi.astype(F32), 0.0)
        tail = jnp.where(row == 1, c_mid.astype(F32), tail)
        tail = jnp.where(row == 2, c_lo.astype(F32), tail)
        both = jnp.concatenate([d_hi, d_lo], axis=0)
        zeros = jnp.zeros((64, AQ), BF16)
        parts = [both, tail.astype(BF16)]
        parts = parts + [zeros] if side == 0 else [zeros] + parts
        dp = mm(va_ref[:, lanes], jnp.concatenate(parts, axis=0))
        ds = (e_ref[slot].astype(F32) * dp).astype(BF16)
        ds_ref[slot] = ds
        dst_ref[slot] = jnp.transpose(ds)
        return both

    def value_grad(p, j, both):
        side, t, slot, h, cols, lanes, hrows, krows, vrows = names(p, j)
        dv = mm(both, et_ref[slot])
        dv = dv[:HD] + dv[HD:]
        if t > 0:
            dv = dv_ref[...] + dv
        if t < NA - 1:
            dv_ref[...] = dv
        else:
            gpT_ref[vrows, :] = dv.astype(BF16)

    def score_grads(p, j):
        side, t, slot, h, cols, lanes, hrows, krows, vrows = names(p, j)
        dq = mm(pT_ref[krows, :], ds_ref[slot])
        gpT_ref[hrows, cols] = (dq * SCALE).astype(BF16)
        dk = mm(pT_ref[hrows, cols], dst_ref[slot])
        if t > 0:
            dk = dk_ref[...] + dk
        if t < NA - 1:
            dk_ref[...] = dk
        else:
            gpT_ref[krows, :] = (dk * SCALE).astype(BF16)

    first_stage(0, 0)
    if LAG:
        ds_ref[1] = jnp.zeros((N, AQ), BF16)
        dst_ref[1] = jnp.zeros((AQ, N), BF16)
        dk_ref[...] = jnp.zeros((HD, N), F32)

    def pair(p, carry):
        for j in range(2 * NA):
            o_un = outputs(p, j)
            if j < 2 * NA - 1:
                first_stage(p, j + 1)
            else:
                first_stage(jnp.minimum(p + 1, H // 2 - 1), 0)
            both = cotangents(p, j, o_un)
            if LAG:
                if j > 0:
                    score_grads(p, j - 1)
                else:
                    score_grads(jnp.maximum(p - 1, 0), 2 * NA - 1)
                value_grad(p, j, both)
            else:
                value_grad(p, j, both)
                score_grads(p, j)
        return carry

    lax.fori_loop(0, H // 2, pair, 0)
    if LAG:
        score_grads(H // 2 - 1, 2 * NA - 1)

    grad_ref[: 3 * C, :] = mm(gpT_ref[...], hid_ref[...]) * POINT_SCALE
    grad_ref[3 * C :, :] = mm(attT_ref[...], og_ref[...]) * POINT_SCALE
    for half in range(2):
        part = grad_ref[:, half * 128 : (half + 1) * 128].reshape(128, 8, 128)
        send_ref[:, half * 8 : (half + 1) * 8, :] = part.astype(BF16)

    gain_sum = jnp.zeros((1, C), F32)
    for t in range(4):
        rows = pl.ds(t * QB, QB)
        att = jnp.transpose(attT_ref[:, rows])
        bo = gath_ref[rows, :].astype(F32) + mm(att, wproj_ref[...])
        bo_ref[pl.ds(t * QB + 8, QB), :] = bo.astype(BF16).astype(F32)
        gp = jnp.transpose(gpT_ref[:, rows])
        gh = mm_nt(gp, wqkv_ref[...])
        normed = normed_ref[rows, :]
        gain_sum = gain_sum + jnp.sum(gh * normed, axis=0, keepdims=True)
        g = gh * gain
        mean_g = jnp.mean(g, axis=1, keepdims=True)
        mean_c = jnp.mean(g * normed, axis=1, keepdims=True)
        dx = og_ref[rows, :].astype(F32) + inv_ref[rows, :] * (g - mean_g - normed * mean_c)
        dx_ref[rows, :] = dx.astype(BF16)
    gain_sum = gain_sum * POINT_SCALE
    gsum_ref[0] = gain_sum[:, :128]
    gsum_ref[1] = gain_sum[:, 128:]
    for t in range(4):
        spot = iota((QB, N), 0) + t * QB
        onehot = jnp.where(spot == serial_row, 1.0, 0.0).astype(BF16)
        gfeats_ref[pl.ds(t * QB, QB), :] = mm(onehot, dx_ref[...]).astype(BF16)

    ids_ref[8 : N + 8, :] = jnp.transpose(
        jnp.broadcast_to(cluster_ref[...].astype(F32), (128, N))
    )
    ids_ref[:8, :] = jnp.full((8, 128), -1.0, F32)
    ids_ref[N + 8 :, :] = jnp.full((8, 128), -2.0, F32)
    bo_ref[:8, :] = jnp.full((8, C), -jnp.inf, F32)
    bo_ref[N + 8 :, :] = jnp.full((8, C), -jnp.inf, F32)
    span = 128
    wide = span + 16

    def pool(i, carry):
        at = pl.multiple_of(i * span, span)
        ids = ids_ref[pl.ds(at, wide), :]
        shifts = (1, 2, 4, wide - 1, wide - 2, wide - 4)
        same = [pltpu.roll(ids, step, 0) == ids for step in shifts]
        for half in range(2):
            cols = slice(half * 128, (half + 1) * 128)
            m = bo_ref[pl.ds(at, wide), cols]
            for step, ok in zip(shifts, same):
                m = jnp.maximum(m, jnp.where(ok, pltpu.roll(m, step, 0), -jnp.inf))
            bo2_ref[pl.ds(at, span), cols] = m[8 : span + 8]
        return carry

    lax.fori_loop(0, N // span, pool, 0)
    pooled_ref[...] = bo2_ref[...].astype(BF16)
    edge_ref[0, :8, :] = bo2_ref[:8, :]
    edge_ref[1, :8, :] = bo2_ref[N - 8 :, :]
    flag = jnp.full((8, C), joined_ref[0], jnp.int32).astype(F32)
    edge_ref[0, 8:, :] = flag
    edge_ref[1, 8:, :] = flag


def local_part(raw, serial, counts, gain, w_qkv, w_proj, out_grad, cluster, joined):
    shapes = (
        jax.ShapeDtypeStruct((N, C), BF16),
        jax.ShapeDtypeStruct((N, C), BF16),
        jax.ShapeDtypeStruct((128, 16, 128), BF16),
        jax.ShapeDtypeStruct((2, 1, 128), F32),
        jax.ShapeDtypeStruct((2, 16, C), F32),
    )
    vm = pl.BlockSpec(memory_space=VMEM)
    sm = pl.BlockSpec(memory_space=pltpu.SMEM)
    return pl.pallas_call(
        local_kernel,
        out_shape=shapes,
        in_specs=[vm, vm, sm, vm, vm, vm, vm, vm, sm],
        out_specs=[vm] * 5,
        scratch_shapes=[
            VMEM((N, C), BF16),
            VMEM((N, C), BF16),
            VMEM((N, C), F32),
            VMEM((N, 1), F32),
            VMEM((3 * C, N), BF16),
            VMEM((C, N), BF16),
            VMEM((N, 4 * C), BF16),
            VMEM((N, 4 * C), BF16),
            VMEM((H * 128, N), BF16),
            VMEM((H * 32, N), BF16),
            VMEM((2, N, AQ), BF16),
            VMEM((2, N, AQ), BF16),
            VMEM((C, N), BF16),
            VMEM((3 * C, N), BF16),
            VMEM((HD, N), F32),
            VMEM((HD, N), F32),
            VMEM((N, C), F32),
            VMEM((N, C), BF16),
            VMEM((N + 16, C), F32),
            VMEM((N, C), F32),
            VMEM((N + 16, 128), F32),
            VMEM((N, 128), F32),
            VMEM((N, 2 * C), BF16),
            VMEM((2, AQ, N), BF16),
            VMEM((2, AQ, N), BF16),
        ],
        compiler_params=pltpu.CompilerParams(vmem_limit_bytes=56 * 1024 * 1024),
        name="local_part",
    )(raw, serial, counts, gain, w_qkv, w_proj, out_grad, cluster, joined)


def comm_kernel(
    send_ref,
    gsum_ref,
    edge_ref,
    ends_in_ref,
    cluster_ref,
    ends_ref,
    gqkv_ref,
    gproj_ref,
    ggain_ref,
    pair_buf,
    pair_gain,
    edge_buf,
    chip_buf,
    chip_gain,
    rs_buf,
    gain_buf,
    ag_buf,
    out_buf,
    gain_out,
    grad_buf,
    sems,
):
    y = lax.axis_index("order_0")
    x = lax.axis_index("order_1")
    core = lax.axis_index("order_2")
    z = lax.axis_index("help")
    chip = (y * 4 + x) * 4 + z
    shard = ((y * 4 + x) * 2 + core) * 4 + z

    def of_shard(s):
        return (s // 32, (s // 8) % 4, (s // 4) % 2, s % 4)

    def of_chip(r):
        return ((y + r // 16) % 4, (x + (r // 4) % 4) % 4, core, (z + r % 4) % 4)

    partner = (y, x, 1 - core, z)
    following = of_shard((shard + 1) % 128)
    previous = of_shard((shard + 127) % 128)

    barrier = pltpu.get_barrier_semaphore()

    def greet(r, carry):
        pl.semaphore_signal(barrier, inc=1, device_id=of_chip(r), device_id_type=MESH)
        return carry

    lax.fori_loop(1, 64, greet, 0)
    for other in (partner, following, previous):
        pl.semaphore_signal(barrier, inc=1, device_id=other, device_id_type=MESH)
    pl.semaphore_wait(barrier, 66)

    def remote(src, dst, i, device):
        return pltpu.make_async_remote_copy(
            src_ref=src,
            dst_ref=dst,
            send_sem=sems.at[2 * i],
            recv_sem=sems.at[2 * i + 1],
            device_id=device,
            device_id_type=MESH,
        )

    far = 64 * (1 - core)
    pair_copy = remote(send_ref.at[pl.ds(far, 64)], pair_buf, 0, partner)
    pair_copy.start()
    pair_gain_copy = remote(gsum_ref.at[1 - core], pair_gain, 1, partner)
    pair_gain_copy.start()
    ahead = remote(edge_ref.at[1], edge_buf.at[0], 2, following)
    ahead.start()
    back = remote(edge_ref.at[0], edge_buf.at[1], 3, previous)
    back.start()

    pair_copy.wait()
    mine = send_ref[pl.ds(64 * core, 64)].astype(F32) + pair_buf[...].astype(F32)
    chip_buf[...] = mine.astype(BF16)
    pair_gain_copy.wait()
    chip_gain[...] = gsum_ref[core] + pair_gain[...]

    def scatter(r, carry):
        to = of_chip(r)
        other = (to[0] * 4 + to[1]) * 4 + to[3]
        remote(chip_buf.at[other], rs_buf.at[chip], 4, to).start()
        remote(chip_gain, gain_buf.at[chip], 5, to).start()
        return carry

    lax.fori_loop(1, 64, scatter, 0)
    rs_buf[pl.ds(chip, 1)] = chip_buf[pl.ds(chip, 1)]
    gain_buf[pl.ds(chip, 1)] = chip_gain[...][None]

    ahead.wait()
    back.wait()
    ids = jnp.transpose(jnp.broadcast_to(cluster_ref[...].astype(F32), (128, N)))
    first = ids[:8]
    last = ids[N - 8 :]
    linked = (edge_ref[0, 8:9, :128] > 0.0) & (shard > 0)
    head_ok = (first == first[:1]) & linked
    next_joined = edge_buf[1, 8:9, :128] > 0.0
    tail_ok = (last == last[7:8]) & next_joined & (shard < 127)
    for half in range(2):
        cols = slice(half * 128, (half + 1) * 128)
        from_prev = edge_buf[0, 7:8, cols]
        from_next = edge_buf[1, 0:1, cols]
        top = edge_ref[0, 0:8, cols]
        top = jnp.where(head_ok, jnp.maximum(top, from_prev), top)
        low = edge_ref[1, 0:8, cols]
        low = jnp.where(tail_ok, jnp.maximum(low, from_next), low)
        above = ends_in_ref[8:16, cols].astype(F32)
        below = ends_in_ref[16:24, cols].astype(F32)
        ends_ref[:16, cols] = jnp.concatenate([top, above], axis=0).astype(BF16)
        ends_ref[16:, cols] = jnp.concatenate([below, low], axis=0).astype(BF16)

    everything = pl.ds(0, 63)
    for i, (src, dst) in ((4, (ag_buf, rs_buf)), (5, (gain_out, gain_buf))):
        whole = remote(dst.at[everything], dst.at[everything], i, partner)
        whole.wait_recv()
        whole.wait_send()
    total = jnp.sum(rs_buf[...].astype(F32), axis=0)
    ag_buf[pl.ds(chip, 1)] = total.astype(BF16)[None]

    def gather(r, carry):
        remote(ag_buf.at[chip], ag_buf.at[chip], 6, of_chip(r)).start()
        return carry

    lax.fori_loop(1, 64, gather, 0)
    gain_out[pl.ds(core, 1)] = jnp.sum(gain_buf[...], axis=0)[None]
    last_gain = remote(gain_out.at[core], gain_out.at[core], 7, partner)
    last_gain.start()
    whole = remote(ag_buf.at[everything], ag_buf.at[everything], 6, partner)
    whole.wait_recv()
    whole.wait_send()
    last_copy = remote(ag_buf, out_buf.at[core], 8, partner)
    last_copy.start()
    out_buf[pl.ds(core, 1)] = ag_buf[...][None]
    last_gain.wait()
    ggain_ref[:, :128] = gain_out[0]
    ggain_ref[:, 128:] = gain_out[1]
    last_copy.wait()
    for c in range(2):
        for half in range(2):
            part = out_buf[c, :, half * 8 : (half + 1) * 8, :].astype(F32).reshape(512, 128)
            grad_buf[c * 512 : (c + 1) * 512, half * 128 : (half + 1) * 128] = part
    gqkv_ref[...] = jnp.transpose(grad_buf[: 3 * C, :])
    gproj_ref[...] = grad_buf[3 * C :, :]


def comm_part(send, gsum, edge, ends, cluster):
    shapes = (
        jax.ShapeDtypeStruct((32, C), BF16),
        jax.ShapeDtypeStruct((C, 3 * C), F32),
        jax.ShapeDtypeStruct((C, C), F32),
        jax.ShapeDtypeStruct((1, C), F32),
    )
    vm = pl.BlockSpec(memory_space=VMEM)
    return pl.pallas_call(
        comm_kernel,
        out_shape=shapes,
        in_specs=[vm] * 5,
        out_specs=[vm] * 4,
        scratch_shapes=[
            VMEM((64, 16, 128), BF16),
            VMEM((1, 128), F32),
            VMEM((2, 16, C), F32),
            VMEM((64, 16, 128), BF16),
            VMEM((1, 128), F32),
            VMEM((64, 16, 128), BF16),
            VMEM((64, 1, 128), F32),
            VMEM((64, 16, 128), BF16),
            VMEM((2, 64, 16, 128), BF16),
            VMEM((2, 1, 128), F32),
            VMEM((N, C), F32),
            pltpu.SemaphoreType.DMA((18,)),
        ],
        compiler_params=pltpu.CompilerParams(
            collective_id=0, has_side_effects=True, vmem_limit_bytes=32 * 1024 * 1024
        ),
        name="comm_part",
    )(send, gsum, edge, ends, cluster)


def body(raw_feats, serial, counts, norm_gain, w_qkv, w_proj, out_grad, cluster, joined):
    pooled, grad_feats, send, gsum, edge = local_part(
        raw_feats[0], serial, counts, norm_gain[None], w_qkv, w_proj, out_grad[0], cluster, joined
    )
    ends = jnp.concatenate([pooled[:16], pooled[N - 16 :]], axis=0)
    ends, grad_qkv, grad_proj, grad_gain = comm_part(send, gsum, edge, ends, cluster)
    pooled = pooled.at[:16].set(ends[:16]).at[N - 16 :].set(ends[16:])
    return (pooled[None], grad_feats[None], grad_qkv, grad_proj, grad_gain[0])


def solution(mesh):
    torus = Mesh(
        mesh.devices.reshape(4, 4, 2, mesh.shape["help"]), ("order_0", "order_1", "order_2", "help")
    )
    placed = (
        P(ORDER_HELP, None, None),
        P(ORDER_HELP, None),
        P(ORDER_HELP, None),
        P(),
        P(),
        P(),
        P(ORDER_HELP, None, None),
        P(ORDER_HELP, None),
        P(ORDER_HELP),
    )
    return jax.shard_map(
        body,
        mesh=torus,
        in_specs=placed,
        out_specs=(P(ORDER_HELP, None, None), P(ORDER_HELP, None, None), P(), P(), P()),
        check_vma=False,
    )
```
